16 devices in a mesh: dp: 4 (over y, z, core), tp: 4 (over x).
Axes of the slice: x: 4, y: 2, z: 1, core: 2. Of those that a mesh axis runs over, the one named last changes fastest.
The devices are a block of a 4x4x8 slice.
Arguments:
- x: bfloat16 [8192, 2048], P('dp'), parts along dimension 0
- dy: bfloat16 [8192, 2048], P('dp'), parts along dimension 0
- gate: bfloat16 [8192, 8192], P('dp', 'tp'), parts along dimension 0
- up: bfloat16 [8192, 8192], P('dp', 'tp'), parts along dimension 0
- w_gate: bfloat16 [2048, 8192], P(None, 'tp')
- w_up: bfloat16 [2048, 8192], P(None, 'tp')
- w_down: bfloat16 [8192, 2048], P('tp')
Outputs:
- output 1: bfloat16 [8192, 2048], P('dp'), parts along dimension 0
- output 2: bfloat16 [8192, 8192], P('dp', 'tp'), parts along dimension 0
- output 3: bfloat16 [8192, 8192], P('dp', 'tp'), parts along dimension 0
- output 4: bfloat16 [32768, 2048], P(('dp', 'tp')), parts along dimension 0
There are 4 independent parts. The reference program is written for one: setup_inputs(seed, part) draws one part's arguments, and reference() takes and returns one part's arrays. A program takes and returns all parts, laid end to end along the dimension named above; an argument that names none is the same for every part.
All inputs are finite; a program needn't handle non-finite values.
Results may differ from the reference program's by a relative error of at most 0.012.
Values are sent between devices in bfloat16 or wider.
A program may use at most 768 MiB of HBM per device.

```python
import jax
import jax.numpy as jnp

ROWS = 2048
D = 2048
FF = 8192


def act(gate, up):
    return jax.nn.silu(gate) * up


def setup_inputs(seed: int = 0, part: int = 0) -> dict:
    kx, ky, ka, kb, kg, ku, kd = jax.random.split(jax.random.key(seed), 7)
    kx, ky, ka, kb = (jax.random.fold_in(k, part) for k in (kx, ky, ka, kb))
    drawn = {
        "x": jax.random.normal(kx, (ROWS, D), jnp.float32),
        "dy": jax.random.normal(ky, (ROWS, D), jnp.float32),
        "gate": jax.random.normal(ka, (ROWS, FF), jnp.float32),
        "up": jax.random.normal(kb, (ROWS, FF), jnp.float32),
        "w_gate": jax.random.normal(kg, (D, FF), jnp.float32) * D**-0.5,
        "w_up": jax.random.normal(ku, (D, FF), jnp.float32) * D**-0.5,
        "w_down": jax.random.normal(kd, (FF, D), jnp.float32) * FF**-0.5,
    }
    return {k: v.astype(jnp.bfloat16) for k, v in drawn.items()}


def reference(x, dy, gate, up, w_gate, w_up, w_down):
    hidden, back = jax.vjp(act, gate.astype(jnp.float32), up.astype(jnp.float32))
    d_hidden = jnp.dot(dy, w_down.T, preferred_element_type=jnp.float32)
    d_gate, d_up = (g.astype(jnp.bfloat16) for g in back(d_hidden))
    dx = jnp.dot(d_gate, w_gate.T, preferred_element_type=jnp.float32) + jnp.dot(d_up, w_up.T, preferred_element_type=jnp.float32)
    dw_gate = jnp.dot(x.T, d_gate, preferred_element_type=jnp.float32)
    dw_up = jnp.dot(x.T, d_up, preferred_element_type=jnp.float32)
    dw_down = jnp.dot(hidden.astype(jnp.bfloat16).T, dy, preferred_element_type=jnp.float32)
    return tuple(g.astype(jnp.bfloat16) for g in (dx, dw_gate, dw_up, dw_down))
```

```python
import functools

import jax
import jax.numpy as jnp
from jax import lax
from jax.experimental import pallas as pl
from jax.experimental.pallas import tpu as pltpu
from jax.sharding import PartitionSpec as P


BF16, F32 = jnp.bfloat16, jnp.float32
NT = (((1,), (1,)), ((), ()))
TN = (((0,), (0,)), ((), ()))
TILE = 512
VMEM_LIMIT = 67043328


def dot(a, b, dims):
    return lax.dot_general(a, b, dims, preferred_element_type=F32)


def reduce_kernel(
    n, dy, gate, up, w_gate, w_up, w_down,
    d_gate, d_up, hidden, sum_a, sum_b,
    wd, wgu, dgu, dyb, gb, ub, hb, first, recv, own,
    wd_sem, wgu_sem, dy_sem, g_sem, u_sem, h_sem, out_sem, fin_sem, send_sem, recv_sem,
):
    rows, width = dyb.shape[1], wd.shape[1]
    units = wd.shape[0]
    half = width // 2
    tiles = units // TILE
    pieces = half // TILE
    me = lax.axis_index("tp")
    right, left = lax.rem(me + 1, n), lax.rem(me + n - 1, n)
    shards = [lax.rem(me + off, n) for off in (3, 2, 0, 1)]
    places = ((0, 0), (1, 2), (0, 0), (2, 1))

    def dy_copy(k):
        src = dy.at[pl.ds(shards[k] * rows, rows), :]
        return pltpu.make_async_copy(src, dyb.at[k % 2], dy_sem.at[k % 2])

    def act_copies(shard, t, slot):
        at = (pl.ds(shard * rows, rows), pl.ds(pl.multiple_of(t * TILE, TILE), TILE))
        return (
            pltpu.make_async_copy(gate.at[at], gb.at[slot], g_sem.at[slot]),
            pltpu.make_async_copy(up.at[at], ub.at[slot], u_sem.at[slot]),
        )

    def hidden_copy(shard, t, slot):
        at = (pl.ds(shard * rows, rows), pl.ds(pl.multiple_of(t * TILE, TILE), TILE))
        return pltpu.make_async_copy(hb.at[slot], hidden.at[at], h_sem.at[slot])

    def wd_copy(t):
        at = pl.ds(pl.multiple_of(t * TILE, TILE), TILE)
        return pltpu.make_async_copy(w_down.at[at, :], wd.at[at, :], wd_sem.at[t])

    def wgu_copies(c):
        at = pl.ds(pl.multiple_of(c * TILE, TILE), TILE)
        return (
            pltpu.make_async_copy(w_gate.at[at, :], wgu.at[at, pl.ds(0, units)], wgu_sem.at[0, c]),
            pltpu.make_async_copy(w_up.at[at, :], wgu.at[at, pl.ds(units, units)], wgu_sem.at[1, c]),
        )

    def out_copies(k):
        at, src = pl.ds(shards[k] * rows, rows), dgu.at[k % (n - 1)]
        return (
            pltpu.make_async_copy(src.at[:, pl.ds(0, units)], d_gate.at[at, :], out_sem.at[0, k]),
            pltpu.make_async_copy(src.at[:, pl.ds(units, units)], d_up.at[at, :], out_sem.at[1, k]),
        )

    def remote(src, hop, way, p):
        return pltpu.make_async_remote_copy(
            src_ref=src,
            dst_ref=recv.at[way, hop, p],
            send_sem=send_sem.at[way, hop, p],
            recv_sem=recv_sem.at[way, hop, p],
            device_id={"tp": lax.rem(me + 1 + way * (n - 2), n)},
            device_id_type=pl.DeviceIdType.MESH,
        )

    dy_copy(0).start()
    wd_copy(0).start()
    for c in act_copies(shards[0], 0, 0):
        c.start()
    for t in range(1, tiles):
        wd_copy(t).start()
    for p in range(pieces):
        for way in range(2):
            for c in wgu_copies(way * pieces + p):
                c.start()

    barrier = pltpu.get_barrier_semaphore()
    for other in (left, right):
        pl.semaphore_signal(barrier, inc=1, device_id={"tp": other}, device_id_type=pl.DeviceIdType.MESH)
    pl.semaphore_wait(barrier, 2)

    def gradients(k):
        dy_copy(k).wait()
        if k + 1 < n:
            dy_copy(k + 1).start()
        else:
            for c in out_copies(0):
                c.wait()

        def tile(t, carry):
            slot = lax.rem(t, 2)
            at = pl.ds(pl.multiple_of(t * TILE, TILE), TILE)
            if k + 1 < n:
                more = lax.rem(t + 1, tiles)
                shard = jnp.where(t + 1 < tiles, shards[k], shards[k + 1])
                for c in act_copies(shard, more, 1 - slot):
                    c.start()
            else:
                @pl.when(t + 1 < tiles)
                def _():
                    for c in act_copies(shards[k], t + 1, 1 - slot):
                        c.start()
            if k == 0:
                wd_copy(t).wait()
            for c in act_copies(shards[k], t, slot):
                c.wait()
            d_hidden = dot(dyb[k % 2], wd[at, :], NT)
            g = gb[slot].astype(F32)
            u = ub[slot].astype(F32)
            s = jax.nn.sigmoid(g)
            silu = g * s
            if k == 0:
                @pl.when(t >= 2)
                def _():
                    hidden_copy(shards[k], t - 2, slot).wait()
            else:
                hidden_copy(shards[k], t, slot).wait()
            hb[slot] = (silu * u).astype(BF16)
            dgu[k % (n - 1), :, at] = (d_hidden * u * (s * (1.0 + g * (1.0 - s)))).astype(BF16)
            dgu[k % (n - 1), :, pl.ds(pl.multiple_of(units + t * TILE, TILE), TILE)] = (d_hidden * silu).astype(BF16)
            hidden_copy(shards[k], t, slot).start()
            return carry

        lax.fori_loop(0, tiles, tile, 0)
        for c in out_copies(k):
            c.start()

    def term(place, way, p):
        c = way * pieces + p
        return dot(dgu[place], wgu[pl.ds(pl.multiple_of(c * TILE, TILE), TILE), :], NT)

    def place_of(hop, way):
        a, b = places[hop]
        return a + way * (b - a)

    gradients(0)

    def hop0(q, carry):
        p, way = q // 2, lax.rem(q, 2)
        for c in wgu_copies(way * pieces + p):
            c.wait()
        first[way, p] = term(0, way, p).astype(BF16)
        remote(first.at[way, p], 0, way, p).start()
        return carry

    lax.fori_loop(0, 2 * pieces, hop0, 0)
    gradients(1)
    gradients(2)

    def later(hop, way, p):
        mine = term(place_of(hop, way), way, p)
        remote(recv.at[way, hop - 1, p], hop - 1, way, p).wait_recv()
        recv[way, hop - 1, p] = (mine + recv[way, hop - 1, p].astype(F32)).astype(BF16)
        remote(recv.at[way, hop - 1, p], hop, way, p).start()

    def hop1(q, carry):
        later(1, lax.rem(q, 2), q // 2)
        return carry

    lax.fori_loop(0, 2 * pieces, hop1, 0)
    gradients(3)

    def hop2(p, carry):
        def send(way, carry):
            later(2, way, p)
            return carry

        def keep(way, carry):
            own[way, p] = term(place_of(3, way), way, p)
            return carry

        lax.fori_loop(0, 2, send, 0)
        lax.fori_loop(0, 2, keep, 0)
        return carry

    lax.fori_loop(0, pieces, hop2, 0)

    def final_copy(way, p):
        out = (sum_a, sum_b)[way]
        return pltpu.make_async_copy(
            recv.at[way, n - 2, p], out.at[:, pl.ds(p * TILE, TILE)], fin_sem.at[way, p]
        )

    for p in range(pieces):
        for way in range(2):
            remote(recv.at[way, n - 2, p], n - 2, way, p).wait_recv()
            recv[way, n - 2, p] = (own[way, p] + recv[way, n - 2, p].astype(F32)).astype(BF16)
            final_copy(way, p).start()
    for t in (tiles - 2, tiles - 1):
        hidden_copy(shards[n - 1], t, t % 2).wait()
    for k in range(1, n):
        for c in out_copies(k):
            c.wait()
    for p in range(pieces):
        for way in range(2):
            remote(first.at[way, p], 0, way, p).wait_send()
            for hop in range(1, n - 1):
                remote(recv.at[way, hop - 1, p], hop, way, p).wait_send()
            final_copy(way, p).wait()


def reduce_scatter(n, dy, gate, up, w_gate, w_up, w_down):
    tokens, width = dy.shape
    units = gate.shape[1]
    rows, half = tokens // n, width // 2
    pieces = half // TILE
    wide = jax.ShapeDtypeStruct((tokens, units), BF16)
    part = jax.ShapeDtypeStruct((rows, half), BF16)
    dma = pltpu.SemaphoreType.DMA
    return pl.pallas_call(
        functools.partial(reduce_kernel, n),
        out_shape=(wide, wide, wide, part, part),
        in_specs=[pl.BlockSpec(memory_space=pl.ANY)] * 6,
        out_specs=[pl.BlockSpec(memory_space=pl.ANY)] * 5,
        scratch_shapes=[
            pltpu.VMEM((units, width), BF16),
            pltpu.VMEM((width, 2 * units), BF16),
            pltpu.VMEM((n - 1, rows, 2 * units), BF16),
            pltpu.VMEM((2, rows, width), BF16),
            pltpu.VMEM((2, rows, TILE), BF16),
            pltpu.VMEM((2, rows, TILE), BF16),
            pltpu.VMEM((2, rows, TILE), BF16),
            pltpu.VMEM((2, pieces, rows, TILE), BF16),
            pltpu.VMEM((2, n - 1, pieces, rows, TILE), BF16),
            pltpu.VMEM((2, pieces, rows, TILE), F32),
            dma((units // TILE,)),
            dma((2, width // TILE)),
            dma((2,)),
            dma((2,)),
            dma((2,)),
            dma((2,)),
            dma((2, n)),
            dma((2, pieces)),
            dma((2, n - 1, pieces)),
            dma((2, n - 1, pieces)),
        ],
        compiler_params=pltpu.CompilerParams(
            collective_id=0, has_side_effects=True, vmem_limit_bytes=VMEM_LIMIT
        ),
        cost_estimate=pl.CostEstimate(
            flops=6 * tokens * width * units, bytes_accessed=72 << 20, transcendentals=0
        ),
        name="reduce",
    )(dy, gate, up, w_gate, w_up, w_down)


def place_copies(n, hop, pieces, dx, bufs, in_sem, out_sem):
    me = lax.axis_index("tp")
    shards = (lax.rem(me + n - hop, n), lax.rem(me + 2 + hop, n))
    rows, half = pieces[0].shape
    ins, outs = [], []
    for way in range(2):
        at = (pl.ds(shards[way] * rows, rows), pl.ds(way * half, half))
        ins.append(pltpu.make_async_copy(pieces[way], bufs.at[way], in_sem.at[way]))
        outs.append(pltpu.make_async_copy(bufs.at[way], dx.at[at], out_sem.at[way]))
    return ins, outs


def weight_kernel(n, hop, a, b, *rest):
    pieces, rest = rest[:2], rest[-5:]
    out, dx, bufs, in_sem, out_sem = rest
    i, j = pl.program_id(0), pl.program_id(1)
    step = i * pl.num_programs(1) + j
    ins, outs = place_copies(n, hop, pieces, dx, bufs, in_sem, out_sem)

    @pl.when(step == 0)
    def _():
        for c in ins:
            c.start()

    @pl.when(step == 2)
    def _():
        for c in ins:
            c.wait()
        for c in outs:
            c.start()

    out[...] = dot(a[...], b[...], TN).astype(BF16)

    @pl.when(step == pl.num_programs(0) * pl.num_programs(1) - 1)
    def _():
        for c in outs:
            c.wait()


def weight_gradient(n, hop, a, b, pieces, dx, name):
    tokens, rows, cols = a.shape[0], a.shape[1], b.shape[1]
    bm, bn = 1024, 512
    anywhere = pl.BlockSpec(memory_space=pl.ANY)
    whole = (tokens, 2 * pieces[0].shape[1])
    args = (a, b, *pieces) + (() if dx is None else (dx,))
    return pl.pallas_call(
        functools.partial(weight_kernel, n, hop),
        grid=(rows // bm, cols // bn),
        out_shape=(jax.ShapeDtypeStruct((rows, cols), BF16), jax.ShapeDtypeStruct(whole, BF16)),
        in_specs=[
            pl.BlockSpec((tokens, bm), lambda i, j: (0, i)),
            pl.BlockSpec((tokens, bn), lambda i, j: (0, j)),
        ]
        + [anywhere] * (len(args) - 2),
        out_specs=[pl.BlockSpec((bm, bn), lambda i, j: (i, j)), anywhere],
        scratch_shapes=[
            pltpu.VMEM((2, *pieces[0].shape), BF16),
            pltpu.SemaphoreType.DMA((2,)),
            pltpu.SemaphoreType.DMA((2,)),
        ],
        input_output_aliases={} if dx is None else {4: 1},
        compiler_params=pltpu.CompilerParams(vmem_limit_bytes=48 << 20),
        cost_estimate=pl.CostEstimate(
            flops=2 * tokens * rows * cols, bytes_accessed=32 << 20, transcendentals=0
        ),
        name=name,
    )(*args)


def finish_kernel(n, hop, a, b, _, dx, bufs, in_sem, out_sem):
    ins, outs = place_copies(n, hop, (a, b), dx, bufs, in_sem, out_sem)
    for c in ins:
        c.start()
    for i, o in zip(ins, outs):
        i.wait()
        o.start()
    for c in outs:
        c.wait()


def finish(n, hop, pieces, dx):
    anywhere = pl.BlockSpec(memory_space=pl.ANY)
    return pl.pallas_call(
        functools.partial(finish_kernel, n, hop),
        out_shape=jax.ShapeDtypeStruct(dx.shape, BF16),
        in_specs=[anywhere] * 3,
        out_specs=anywhere,
        scratch_shapes=[
            pltpu.VMEM((2, *pieces[0].shape), BF16),
            pltpu.SemaphoreType.DMA((2,)),
            pltpu.SemaphoreType.DMA((2,)),
        ],
        input_output_aliases={2: 0},
        name="finish",
    )(*pieces, dx)


def solution(mesh):
    n = mesh.shape["tp"]
    to_right = [(i, (i + 1) % n) for i in range(n)]
    to_left = [(i, (i - 1) % n) for i in range(n)]

    def step(x, dy, gate, up, w_gate, w_up, w_down):
        d_gate, d_up, hidden, *pieces = reduce_scatter(n, dy, gate, up, w_gate, w_up, w_down)
        dx, grads = None, []
        for hop, (a, b) in enumerate(((x, d_gate), (x, d_up), (hidden, dy))):
            onward = [lax.ppermute(p, "tp", ways) for p, ways in zip(pieces, (to_right, to_left))]
            grad, dx = weight_gradient(n, hop, a, b, pieces, dx, f"weight{hop}")
            grads.append(grad)
            pieces = onward
        dx = finish(n, n - 1, pieces, dx)
        return dx, *grads

    tokens, columns, rows = P("dp", None), P(None, "tp"), P("tp", None)
    return jax.shard_map(
        step,
        mesh=mesh,
        in_specs=(tokens, tokens, P("dp", "tp"), P("dp", "tp"), columns, columns, rows),
        out_specs=(tokens, P("dp", "tp"), P("dp", "tp"), P(("dp", "tp"), None)),
        check_vma=False,
    )
```

```python
import functools

import jax
import jax.numpy as jnp
from jax import lax
from jax.experimental import pallas as pl
from jax.experimental.pallas import tpu as pltpu
from jax.sharding import PartitionSpec as P


BF16, F32 = jnp.bfloat16, jnp.float32
NT = (((1,), (1,)), ((), ()))
TN = (((0,), (0,)), ((), ()))
TILE = 512
PART = TILE // 2
STRIP = 16
WIDE = 512
FIRST = 4
VMEM_LIMIT = 67043328


def dot(a, b, dims):
    return lax.dot_general(a, b, dims, preferred_element_type=F32)


def reduce_kernel(
    n, dy, gate, up, w_gate, w_up, w_down,
    d_gate, d_up, hidden, sum_a, sum_b,
    wd, wgu, dgu, dyb, gb, ub, acc_a, acc_b, first, recv, own,
    wd_sem, wgu_sem, dy_sem, g_sem, u_sem, h_sem, out_sem, fin_sem, send_sem, recv_sem,
):
    rows, width = dyb.shape[1], wd.shape[1]
    units = wd.shape[0]
    half = width // 2
    tiles = units // TILE
    pieces = half // TILE
    me = lax.axis_index("tp")
    right, left = lax.rem(me + 1, n), lax.rem(me + n - 1, n)
    places = ((0, 0), (1, 2), (0, 0), (2, 1))

    def rows_of(k):
        if isinstance(k, int):
            return pl.ds(lax.rem(me + (3, 2, 0, 1)[k], n) * rows, rows)
        return pl.ds(lax.rem(me + n - 2 * k, n) * rows, rows)

    def tile_at(t):
        return pl.ds(pl.multiple_of(t * TILE, TILE), TILE)

    def dy_copy(k):
        slot = lax.rem(k, 2)
        return pltpu.make_async_copy(dy.at[rows_of(k), :], dyb.at[slot], dy_sem.at[slot])

    def act_copies(k, t):
        slot, at = lax.rem(k, 2), tile_at(t)
        return (
            pltpu.make_async_copy(gate.at[rows_of(k), at], gb.at[slot, :, at], g_sem.at[slot, t]),
            pltpu.make_async_copy(up.at[rows_of(k), at], ub.at[slot, :, at], u_sem.at[slot, t]),
        )

    def fetch(k):
        dy_copy(k).start()
        for t in range(tiles):
            for c in act_copies(k, t):
                c.start()

    def hidden_copy(k):
        slot = lax.rem(k, 2)
        return pltpu.make_async_copy(gb.at[slot], hidden.at[rows_of(k), :], h_sem.at[slot])

    def wd_copy(t):
        at = pl.ds(pl.multiple_of(t * TILE, TILE), TILE)
        return pltpu.make_async_copy(w_down.at[at, :], wd.at[at, :], wd_sem.at[t])

    def wgu_copies(c):
        at = pl.ds(pl.multiple_of(c * TILE, TILE), TILE)
        return (
            pltpu.make_async_copy(w_gate.at[at, :], wgu.at[at, pl.ds(0, units)], wgu_sem.at[0, c]),
            pltpu.make_async_copy(w_up.at[at, :], wgu.at[at, pl.ds(units, units)], wgu_sem.at[1, c]),
        )

    def out_copies(k):
        slot = lax.rem(k, n - 1)
        src = dgu.at[slot]
        return (
            pltpu.make_async_copy(src.at[:, pl.ds(0, units)], d_gate.at[rows_of(k), :], out_sem.at[0, slot]),
            pltpu.make_async_copy(src.at[:, pl.ds(units, units)], d_up.at[rows_of(k), :], out_sem.at[1, slot]),
        )

    def remote(src, hop, way, p):
        return pltpu.make_async_remote_copy(
            src_ref=src,
            dst_ref=recv.at[way, hop, p],
            send_sem=send_sem.at[way, hop, p],
            recv_sem=recv_sem.at[way, hop, p],
            device_id={"tp": lax.rem(me + 1 + way * (n - 2), n)},
            device_id_type=pl.DeviceIdType.MESH,
        )

    dy_copy(0).start()
    wd_copy(0).start()

    barrier = pltpu.get_barrier_semaphore()
    for other in (left, right):
        pl.semaphore_signal(barrier, inc=1, device_id={"tp": other}, device_id_type=pl.DeviceIdType.MESH)
    pl.semaphore_wait(barrier, 2)

    def weights(q):
        for c in wgu_copies(lax.rem(q, 2) * pieces + q // 2):
            c.start()

    def gradients(k):
        side, slot = lax.rem(k, 2), lax.rem(k, n - 1)

        def product(acc, t, part):
            at = pl.ds(pl.multiple_of(t * TILE + part * PART, PART), PART)
            acc[...] = dot(dyb[side], wd[at, :], NT)

        def finish(acc, t, part):
            start = t * TILE + part * PART
            at = pl.ds(pl.multiple_of(start, PART), PART)
            for r in range(0, rows, STRIP):
                row = pl.ds(r, STRIP)
                g = gb[side, row, at].astype(F32)
                u = ub[side, row, at].astype(F32)
                d_hidden = acc[row, :]
                sig = 1.0 / (1.0 + jnp.exp(-g))
                silu = g * sig
                gb[side, row, at] = (silu * u).astype(BF16)
                dgu[slot, row, at] = (d_hidden * u * (sig + silu * (1.0 - sig))).astype(BF16)
                dgu[slot, row, pl.ds(pl.multiple_of(units + start, PART), PART)] = (d_hidden * silu).astype(BF16)

        def ready(t):
            for c in act_copies(k, t):
                c.wait()

        def tile(t, carry):
            if isinstance(k, int) and k == 0:
                wd_copy(t + 1).wait()
                ready(t)
                for c in act_copies(k, t + 1):
                    c.start()

                @pl.when(t + 2 < tiles)
                def _():
                    wd_copy(t + 2).start()

                @pl.when(t >= 1)
                def _():
                    weights(t - 1)
            else:
                ready(t)
            product(acc_b, t, 1)
            finish(acc_a, t, 0)
            product(acc_a, t + 1, 0)
            finish(acc_b, t, 1)
            return carry

        dy_copy(k).wait()
        if isinstance(k, int) and k == 0:
            wd_copy(0).wait()
            wd_copy(1).start()
            for c in act_copies(k, 0):
                c.start()
        product(acc_a, 0, 0)
        lax.fori_loop(0, tiles - 1, tile, 0)
        if isinstance(k, int) and k == 0:
            for q in range(tiles - 2, 2 * pieces):
                weights(q)
        ready(tiles - 1)
        product(acc_b, tiles - 1, 1)
        finish(acc_a, tiles - 1, 0)
        finish(acc_b, tiles - 1, 1)
        if isinstance(k, int) and k == 0:
            fetch(1)
        hidden_copy(k).start()
        for c in out_copies(k):
            c.start()

    def term(place, way, p, out):
        c = way * pieces + p
        for part, ref in enumerate(out):
            at = pl.ds(pl.multiple_of(c * TILE + part * PART, PART), PART)
            ref[...] = dot(dgu[place], wgu[at, :], NT)

    def round_to(ref, mine, old=None):
        for part, acc in enumerate(mine):
            cols = pl.ds(part * PART, PART)
            for r in range(0, rows, STRIP):
                row = pl.ds(r, STRIP)
                value = acc[row, :]
                if old is not None:
                    value = value + old[row, cols].astype(F32)
                ref[row, cols] = value.astype(BF16)

    def place_of(hop, way):
        a, b = places[hop]
        return a + way * (b - a)

    gradients(0)

    def hop0(q, carry):
        p, way = q // 2, lax.rem(q, 2)
        for c in wgu_copies(way * pieces + p):
            c.wait()
        term(0, way, p, (acc_a, acc_b))
        round_to(first.at[way, p], (acc_a, acc_b))
        remote(first.at[way, p], 0, way, p).start()
        return carry

    lax.fori_loop(0, 2 * pieces, hop0, 0)
    hidden_copy(0).wait()
    fetch(2)

    def middle(k, carry):
        gradients(k)
        return carry

    lax.fori_loop(1, n - 1, middle, 0)
    hidden_copy(1).wait()
    fetch(3)

    def later(hop, way, p):
        term(place_of(hop, way), way, p, (acc_a, acc_b))
        remote(recv.at[way, hop - 1, p], hop - 1, way, p).wait_recv()
        round_to(recv.at[way, hop - 1, p], (acc_a, acc_b), recv.at[way, hop - 1, p])
        remote(recv.at[way, hop - 1, p], hop, way, p).start()

    def hop1(q, carry):
        later(1, lax.rem(q, 2), q // 2)
        return carry

    lax.fori_loop(0, 2 * pieces, hop1, 0)
    for c in out_copies(0):
        c.wait()
    gradients(3)

    def hop2(q, carry):
        later(2, lax.rem(q, 2), q // 2)
        return carry

    lax.fori_loop(0, 2 * pieces, hop2, 0)

    def final_copy(way, p):
        out = (sum_a, sum_b)[way]
        return pltpu.make_async_copy(
            recv.at[way, n - 2, p], out.at[:, pl.ds(p * TILE, TILE)], fin_sem.at[way, p]
        )

    def close(way, p, mine):
        last = recv.at[way, n - 2, p]
        remote(last, n - 2, way, p).wait_recv()
        round_to(last, mine, last)
        final_copy(way, p).start()

    def keep(way, carry):
        term(place_of(n - 1, way), way, pieces - 1, (own.at[way, 0], own.at[way, 1]))
        return carry

    lax.fori_loop(0, 2, keep, 0)
    for p in range(pieces):
        for way in range(2):
            if p < pieces - 1:
                term(place_of(n - 1, way), way, p, (acc_a, acc_b))
                close(way, p, (acc_a, acc_b))
            else:
                close(way, p, (own.at[way, 0], own.at[way, 1]))
    for k in (n - 2, n - 1):
        hidden_copy(k).wait()
    for k in range(1, n):
        for c in out_copies(k):
            c.wait()
    for p in range(pieces):
        for way in range(2):
            remote(first.at[way, p], 0, way, p).wait_send()
            for hop in range(1, n - 1):
                remote(recv.at[way, hop - 1, p], hop, way, p).wait_send()
            final_copy(way, p).wait()


def reduce_scatter(n, dy, gate, up, w_gate, w_up, w_down):
    tokens, width = dy.shape
    units = gate.shape[1]
    rows, half = tokens // n, width // 2
    pieces = half // TILE
    wide = jax.ShapeDtypeStruct((tokens, units), BF16)
    part = jax.ShapeDtypeStruct((rows, half), BF16)
    dma = pltpu.SemaphoreType.DMA
    return pl.pallas_call(
        functools.partial(reduce_kernel, n),
        out_shape=(wide, wide, wide, part, part),
        in_specs=[pl.BlockSpec(memory_space=pltpu.MemorySpace.HBM)] * 6,
        out_specs=[pl.BlockSpec(memory_space=pltpu.MemorySpace.HBM)] * 5,
        scratch_shapes=[
            pltpu.VMEM((units, width), BF16),
            pltpu.VMEM((width, 2 * units), BF16),
            pltpu.VMEM((n - 1, rows, 2 * units), BF16),
            pltpu.VMEM((2, rows, width), BF16),
            pltpu.VMEM((2, rows, units), BF16),
            pltpu.VMEM((2, rows, units), BF16),
            pltpu.VMEM((rows, PART), F32),
            pltpu.VMEM((rows, PART), F32),
            pltpu.VMEM((2, pieces, rows, TILE), BF16),
            pltpu.VMEM((2, n - 1, pieces, rows, TILE), BF16),
            pltpu.VMEM((2, 2, rows, PART), F32),
            dma((units // TILE,)),
            dma((2, width // TILE)),
            dma((2,)),
            dma((2, units // TILE)),
            dma((2, units // TILE)),
            dma((2,)),
            dma((2, n - 1)),
            dma((2, pieces)),
            dma((2, n - 1, pieces)),
            dma((2, n - 1, pieces)),
        ],
        compiler_params=pltpu.CompilerParams(
            collective_id=0, has_side_effects=True, vmem_limit_bytes=VMEM_LIMIT
        ),
        cost_estimate=pl.CostEstimate(
            flops=6 * tokens * width * units, bytes_accessed=72 << 20, transcendentals=0
        ),
        name="reduce",
    )(dy, gate, up, w_gate, w_up, w_down)


def place_copies(n, hop, pieces, dx, bufs, in_sem, out_sem):
    me = lax.axis_index("tp")
    shards = (lax.rem(me + n - hop, n), lax.rem(me + 2 + hop, n))
    rows, half = pieces[0].shape
    ins, outs = [], []
    for way in range(2):
        at = (pl.ds(shards[way] * rows, rows), pl.ds(way * half, half))
        ins.append(pltpu.make_async_copy(pieces[way], bufs.at[way], in_sem.at[way]))
        outs.append(pltpu.make_async_copy(bufs.at[way], dx.at[at], out_sem.at[way]))
    return ins, outs


def weight_kernel(n, hop, a, b, *rest):
    pieces, rest = rest[:2], rest[-12:]
    out, dx, av, bv, ov, acc, bufs, first_sem, b_sem, o_sem, in_sem, out_sem = rest
    depth, height, cols = av.shape[0], av.shape[1] // 2, ov.shape[2]
    chunk = depth // FIRST
    blocks = bv.shape[1] // cols
    ins, outs = place_copies(n, hop, pieces, dx, bufs, in_sem, out_sem)

    def first_copies(k):
        row = pl.ds(k * chunk, chunk)
        ha, hb = (row, pl.ds(0, height)), (row, pl.ds(0, cols))
        return (
            pltpu.make_async_copy(a.at[ha], av.at[ha], first_sem.at[0, k]),
            pltpu.make_async_copy(b.at[hb], bv.at[hb], first_sem.at[1, k]),
        )

    def b_copy(j):
        at = (slice(None), pl.ds(pl.multiple_of(j * cols, cols), cols))
        return pltpu.make_async_copy(b.at[at], bv.at[at], b_sem.at[j])

    def a_copy():
        at = (slice(None), pl.ds(height, height))
        return pltpu.make_async_copy(a.at[at], av.at[at], b_sem.at[0])

    def out_copy(block):
        i, j = block // blocks, lax.rem(block, blocks)
        at = (pl.ds(pl.multiple_of(i * height, height), height), pl.ds(pl.multiple_of(j * cols, cols), cols))
        slot = lax.rem(block, 2)
        return pltpu.make_async_copy(ov.at[slot], out.at[at], o_sem.at[slot])

    for k in range(2):
        for c in first_copies(k):
            c.start()
    for k in range(FIRST):
        for c in first_copies(k):
            c.wait()
        if k + 2 < FIRST:
            for c in first_copies(k + 2):
                c.start()
        elif k + 2 == FIRST:
            for j in range(1, blocks):
                b_copy(j).start()
        else:
            a_copy().start()
            for c in ins:
                c.start()
        row = pl.ds(k * chunk, chunk)
        part = dot(av[row, pl.ds(0, height)], bv[row, pl.ds(0, cols)], TN)
        if k == 0:
            acc[...] = part
        elif k + 1 < FIRST:
            acc[...] += part
        else:
            ov[0] = (acc[...] + part).astype(BF16)
    out_copy(0).start()

    def step(block, carry):
        i, j = block // blocks, lax.rem(block, blocks)

        @pl.when(block < blocks)
        def _():
            b_copy(j).wait()

        @pl.when(block == blocks)
        def _():
            a_copy().wait()
            for c in ins:
                c.wait()
            for c in outs:
                c.start()

        @pl.when(block >= 2)
        def _():
            out_copy(block - 2).wait()

        ha = pl.ds(pl.multiple_of(i * height, height), height)
        hb = pl.ds(pl.multiple_of(j * cols, cols), cols)
        ov[lax.rem(block, 2)] = dot(av[:, ha], bv[:, hb], TN).astype(BF16)
        out_copy(block).start()
        return carry

    lax.fori_loop(1, 2 * blocks, step, 0)
    for block in (2 * blocks - 2, 2 * blocks - 1):
        out_copy(block).wait()
    for c in outs:
        c.wait()


def weight_gradient(n, hop, a, b, pieces, dx, name):
    tokens, rows, cols = a.shape[0], a.shape[1], b.shape[1]
    anywhere = pl.BlockSpec(memory_space=pltpu.MemorySpace.HBM)
    whole = (tokens, 2 * pieces[0].shape[1])
    args = (a, b, *pieces) + (() if dx is None else (dx,))
    dma = pltpu.SemaphoreType.DMA
    return pl.pallas_call(
        functools.partial(weight_kernel, n, hop),
        out_shape=(jax.ShapeDtypeStruct((rows, cols), BF16), jax.ShapeDtypeStruct(whole, BF16)),
        in_specs=[anywhere] * len(args),
        out_specs=[anywhere] * 2,
        scratch_shapes=[
            pltpu.VMEM((tokens, rows), BF16),
            pltpu.VMEM((tokens, cols), BF16),
            pltpu.VMEM((2, rows // 2, WIDE), BF16),
            pltpu.VMEM((rows // 2, WIDE), F32),
            pltpu.VMEM((2, *pieces[0].shape), BF16),
            dma((2, FIRST)),
            dma((cols // WIDE,)),
            dma((2,)),
            dma((2,)),
            dma((2,)),
        ],
        input_output_aliases={} if dx is None else {4: 1},
        compiler_params=pltpu.CompilerParams(vmem_limit_bytes=VMEM_LIMIT),
        cost_estimate=pl.CostEstimate(
            flops=2 * tokens * rows * cols, bytes_accessed=32 << 20, transcendentals=0
        ),
        name=name,
    )(*args)


def finish_kernel(n, hop, a, b, _, dx, bufs, in_sem, out_sem):
    ins, outs = place_copies(n, hop, (a, b), dx, bufs, in_sem, out_sem)
    for c in ins:
        c.start()
    for i, o in zip(ins, outs):
        i.wait()
        o.start()
    for c in outs:
        c.wait()


def finish(n, hop, pieces, dx):
    anywhere = pl.BlockSpec(memory_space=pltpu.MemorySpace.HBM)
    return pl.pallas_call(
        functools.partial(finish_kernel, n, hop),
        out_shape=jax.ShapeDtypeStruct(dx.shape, BF16),
        in_specs=[anywhere] * 3,
        out_specs=anywhere,
        scratch_shapes=[
            pltpu.VMEM((2, *pieces[0].shape), BF16),
            pltpu.SemaphoreType.DMA((2,)),
            pltpu.SemaphoreType.DMA((2,)),
        ],
        input_output_aliases={2: 0},
        compiler_params=pltpu.CompilerParams(vmem_limit_bytes=VMEM_LIMIT),
        name="finish",
    )(*pieces, dx)


def solution(mesh):
    n = mesh.shape["tp"]
    to_right = [(i, (i + 1) % n) for i in range(n)]
    to_left = [(i, (i - 1) % n) for i in range(n)]

    def step(x, dy, gate, up, w_gate, w_up, w_down):
        d_gate, d_up, hidden, *pieces = reduce_scatter(n, dy, gate, up, w_gate, w_up, w_down)
        dx, grads = None, []
        for hop, (a, b) in enumerate(((x, d_gate), (x, d_up), (hidden, dy))):
            onward = [lax.ppermute(p, "tp", ways) for p, ways in zip(pieces, (to_right, to_left))]
            grad, dx = weight_gradient(n, hop, a, b, pieces, dx, f"weight{hop}")
            grads.append(grad)
            pieces = onward
        dx = finish(n, n - 1, pieces, dx)
        return dx, *grads

    tokens, columns, rows = P("dp", None), P(None, "tp"), P("tp", None)
    return jax.shard_map(
        step,
        mesh=mesh,
        in_specs=(tokens, tokens, P("dp", "tp"), P("dp", "tp"), columns, columns, rows),
        out_specs=(tokens, P("dp", "tp"), P("dp", "tp"), P(("dp", "tp"), None)),
        check_vma=False,
    )
```

```python
import functools

import jax
import jax.numpy as jnp
from jax import lax
from jax.experimental import pallas as pl
from jax.experimental.pallas import tpu as pltpu
from jax.sharding import PartitionSpec as P


BF16, F32 = jnp.bfloat16, jnp.float32
NT = (((1,), (1,)), ((), ()))
TN = (((0,), (0,)), ((), ()))
TILE = 512
STRIP = 16
WIDE = 512
FIRST = 4
VMEM_LIMIT = 67043328


def dot(a, b, dims):
    return lax.dot_general(a, b, dims, preferred_element_type=F32)


def reduce_kernel(
    n, dy, gate, up, w_gate, w_up, w_down,
    d_gate, d_up, hidden, sum_a, sum_b,
    wd, wgu, dgu, dyb, gb, ub, acc_a, acc_b, first, recv, own,
    wd_sem, wgu_sem, dy_sem, g_sem, u_sem, h_sem, out_sem, fin_sem, send_sem, recv_sem,
):
    rows, width = dyb.shape[1], wd.shape[1]
    half_rows = rows // 2
    units = wd.shape[0]
    tiles = units // TILE
    pieces = width // 2 // TILE
    me = lax.axis_index("tp")
    right, left = lax.rem(me + 1, n), lax.rem(me + n - 1, n)
    places = ((0, 0), (1, 2), (0, 0), (2, 1))

    def half(h):
        return pl.ds(pl.multiple_of(h * half_rows, half_rows), half_rows)

    def rows_of(k, h):
        shard = lax.rem(me + (3, 2, 0, 1)[k], n) if isinstance(k, int) else lax.rem(me + n - 2 * k, n)
        return pl.ds(pl.multiple_of(shard * rows + h * half_rows, half_rows), half_rows)

    def tile_at(t):
        return pl.ds(pl.multiple_of(t * TILE, TILE), TILE)

    def dy_copy(k, h):
        side = lax.rem(k, 2)
        return pltpu.make_async_copy(dy.at[rows_of(k, h), :], dyb.at[side, half(h), :], dy_sem.at[side, h])

    def act_copies(k, h, t):
        side, at = lax.rem(k, 2), tile_at(t)
        return (
            pltpu.make_async_copy(gate.at[rows_of(k, h), at], gb.at[side, half(h), at], g_sem.at[side, h, t]),
            pltpu.make_async_copy(up.at[rows_of(k, h), at], ub.at[side, half(h), at], u_sem.at[side, h, t]),
        )

    def fetch(k, h):
        dy_copy(k, h).start()
        for t in range(tiles):
            for c in act_copies(k, h, t):
                c.start()

    def hidden_copy(k, h):
        side = lax.rem(k, 2)
        return pltpu.make_async_copy(gb.at[side, half(h), :], hidden.at[rows_of(k, h), :], h_sem.at[side, h])

    def out_copies(k, h):
        slot = lax.rem(k, n - 1)
        return tuple(
            pltpu.make_async_copy(
                dgu.at[slot, half(h), pl.ds(i * units, units)], out.at[rows_of(k, h), :], out_sem.at[i, slot, h]
            )
            for i, out in enumerate((d_gate, d_up))
        )

    def flush(k, h):
        hidden_copy(k, h).start()
        for c in out_copies(k, h):
            c.start()

    def wd_copy(t):
        at = tile_at(t)
        return pltpu.make_async_copy(w_down.at[at, :], wd.at[at, :], wd_sem.at[t])

    def wgu_copies(q):
        c = lax.rem(q, 2) * pieces + q // 2
        at = tile_at(c)
        return (
            pltpu.make_async_copy(w_gate.at[at, :], wgu.at[at, pl.ds(0, units)], wgu_sem.at[0, c]),
            pltpu.make_async_copy(w_up.at[at, :], wgu.at[at, pl.ds(units, units)], wgu_sem.at[1, c]),
        )

    def weights(q):
        for c in wgu_copies(q):
            c.start()

    def remote(src, hop, way, m):
        return pltpu.make_async_remote_copy(
            src_ref=src,
            dst_ref=recv.at[way, hop, m],
            send_sem=send_sem.at[way, hop, m],
            recv_sem=recv_sem.at[way, hop, m],
            device_id={"tp": lax.rem(me + 1 + way * (n - 2), n)},
            device_id_type=pl.DeviceIdType.MESH,
        )

    dy_copy(0, 0).start()
    for t in range(2):
        wd_copy(t).start()
    for c in act_copies(0, 0, 0):
        c.start()

    barrier = pltpu.get_barrier_semaphore()
    for other in (left, right):
        pl.semaphore_signal(barrier, inc=1, device_id={"tp": other}, device_id_type=pl.DeviceIdType.MESH)
    pl.semaphore_wait(barrier, 2)

    def gradients(k, h):
        side, slot = lax.rem(k, 2), lax.rem(k, n - 1)
        opening = isinstance(k, int) and k == 0
        accs = (acc_a, acc_b)

        def product(t):
            accs[t % 2][...] = dot(dyb[side, half(h), :], wd[t * TILE : (t + 1) * TILE, :], NT)

        def finish(t):
            cols, more = pl.ds(t * TILE, TILE), pl.ds(units + t * TILE, TILE)
            for r in range(0, half_rows, STRIP):
                row = pl.ds(pl.multiple_of(h * half_rows + r, STRIP), STRIP)
                g = gb[side, row, cols].astype(F32)
                u = ub[side, row, cols].astype(F32)
                d_hidden = accs[t % 2][r : r + STRIP, :]
                sig = 1.0 / (1.0 + jnp.exp(-g))
                silu = g * sig
                gb[side, row, cols] = (silu * u).astype(BF16)
                dgu[slot, row, cols] = (d_hidden * u * (sig + silu * (1.0 - sig))).astype(BF16)
                dgu[slot, row, more] = (d_hidden * silu).astype(BF16)

        def arrive(t):
            @pl.when(h == 0)
            def _():
                wd_copy(t).wait()
                if t + 2 < tiles:
                    wd_copy(t + 2).start()
                else:
                    weights(t + 2 - tiles)
                if t + 1 < tiles:
                    for c in act_copies(k, 0, t + 1):
                        c.start()

        def ready(t):
            for c in act_copies(k, h, t):
                c.wait()

        dy_copy(k, h).wait()
        if not opening:
            for t in range(tiles):
                ready(t)
        for t in range(tiles):
            if opening:
                arrive(t)
                if t > 0:
                    ready(t - 1)
            product(t)
            if t > 0:
                finish(t - 1)
        if opening:
            ready(tiles - 1)
        finish(tiles - 1)

    def term(hop, way, h, c, out):
        a, b = places[hop]
        at = pl.ds(pl.multiple_of((way * pieces + c) * TILE, TILE), TILE)
        out[...] = dot(dgu[a + way * (b - a), half(h), :], wgu[at, :], NT)

    def round_to(ref, mine, old=None):
        for r in range(0, half_rows, STRIP):
            row = pl.ds(r, STRIP)
            value = mine[row, :]
            if old is not None:
                value = value + old[row, :].astype(F32)
            ref[row, :] = value.astype(BF16)

    def later(hop, way, h, c):
        m = h * pieces + c
        here = recv.at[way, hop - 1, m]
        term(hop, way, h, c, acc_a)
        remote(here, hop - 1, way, m).wait_recv()
        round_to(here, acc_a, here)
        remote(here, hop, way, m).start()

    def hop0(h, carry):
        gradients(0, h)

        @pl.when(h == 0)
        def _():
            for q in range(2, 2 * pieces):
                weights(q)
            fetch(0, 1)

        @pl.when(h == 1)
        def _():
            fetch(1, 0)
            fetch(1, 1)

        def message(q, carry):
            way, c = lax.rem(q, 2), q // 2

            @pl.when(h == 0)
            def _():
                for copy in wgu_copies(q):
                    copy.wait()

            m = h * pieces + c
            term(0, way, h, c, acc_a)
            round_to(first.at[way, m], acc_a)
            remote(first.at[way, m], 0, way, m).start()
            return carry

        lax.fori_loop(0, 2 * pieces, message, 0)
        flush(0, h)
        return carry

    lax.fori_loop(0, 2, hop0, 0)
    for h in range(2):
        hidden_copy(0, h).wait()
        fetch(2, h)

    def hop1(h, carry):
        def shard(k, carry):
            gradients(k, h)

            def message(c, carry):
                later(1, k - 1, h, c)
                return carry

            lax.fori_loop(0, pieces, message, 0)
            flush(k, h)
            return carry

        lax.fori_loop(1, n - 1, shard, 0)
        hidden_copy(1, h).wait()
        fetch(3, h)
        return carry

    lax.fori_loop(0, 2, hop1, 0)
    for h in range(2):
        for c in out_copies(0, h):
            c.wait()

    def hop2(h, carry):
        gradients(3, h)

        def message(q, carry):
            later(2, lax.rem(q, 2), h, q // 2)
            return carry

        lax.fori_loop(0, 2 * pieces, message, 0)
        flush(3, h)
        return carry

    lax.fori_loop(0, 2, hop2, 0)

    def final_copy(way, h, c):
        out = (sum_a, sum_b)[way]
        m = h * pieces + c
        return pltpu.make_async_copy(
            recv.at[way, n - 2, m], out.at[half(h), tile_at(c)], fin_sem.at[way, m]
        )

    def close(way, h, c, mine):
        m = h * pieces + c
        last = recv.at[way, n - 2, m]
        remote(last, n - 2, way, m).wait_recv()
        round_to(last, mine, last)
        final_copy(way, h, c).start()

    def keep(q, carry):
        way, c = lax.rem(q, 2), q // 2
        term(n - 1, way, 1, c, own.at[way, c])
        return carry

    lax.fori_loop(0, 2 * pieces, keep, 0)

    def early(c, carry):
        for way in range(2):
            term(n - 1, way, 0, c, acc_a)
            close(way, 0, c, acc_a)
        return carry

    lax.fori_loop(0, pieces, early, 0)

    def late(c, carry):
        for way in range(2):
            close(way, 1, c, own.at[way, c])
        return carry

    lax.fori_loop(0, pieces, late, 0)
    for h in range(2):
        for k in (n - 2, n - 1):
            hidden_copy(k, h).wait()
        for k in range(1, n):
            for c in out_copies(k, h):
                c.wait()
        for c in range(pieces):
            m = h * pieces + c
            for way in range(2):
                remote(first.at[way, m], 0, way, m).wait_send()
                for hop in range(1, n - 1):
                    remote(recv.at[way, hop - 1, m], hop, way, m).wait_send()
                final_copy(way, h, c).wait()


def reduce_scatter(n, dy, gate, up, w_gate, w_up, w_down):
    tokens, width = dy.shape
    units = gate.shape[1]
    rows, half = tokens // n, width // 2
    pieces = half // TILE
    block = (rows // 2, TILE)
    wide = jax.ShapeDtypeStruct((tokens, units), BF16)
    part = jax.ShapeDtypeStruct((rows, half), BF16)
    dma = pltpu.SemaphoreType.DMA
    return pl.pallas_call(
        functools.partial(reduce_kernel, n),
        out_shape=(wide, wide, wide, part, part),
        in_specs=[pl.BlockSpec(memory_space=pltpu.MemorySpace.HBM)] * 6,
        out_specs=[pl.BlockSpec(memory_space=pltpu.MemorySpace.HBM)] * 5,
        scratch_shapes=[
            pltpu.VMEM((units, width), BF16),
            pltpu.VMEM((width, 2 * units), BF16),
            pltpu.VMEM((n - 1, rows, 2 * units), BF16),
            pltpu.VMEM((2, rows, width), BF16),
            pltpu.VMEM((2, rows, units), BF16),
            pltpu.VMEM((2, rows, units), BF16),
            pltpu.VMEM(block, F32),
            pltpu.VMEM(block, F32),
            pltpu.VMEM((2, 2 * pieces, *block), BF16),
            pltpu.VMEM((2, n - 1, 2 * pieces, *block), BF16),
            pltpu.VMEM((2, pieces, *block), F32),
            dma((units // TILE,)),
            dma((2, width // TILE)),
            dma((2, 2)),
            dma((2, 2, units // TILE)),
            dma((2, 2, units // TILE)),
            dma((2, 2)),
            dma((2, n - 1, 2)),
            dma((2, 2 * pieces)),
            dma((2, n - 1, 2 * pieces)),
            dma((2, n - 1, 2 * pieces)),
        ],
        compiler_params=pltpu.CompilerParams(
            collective_id=0, has_side_effects=True, vmem_limit_bytes=VMEM_LIMIT
        ),
        cost_estimate=pl.CostEstimate(
            flops=6 * tokens * width * units, bytes_accessed=72 << 20, transcendentals=0
        ),
        name="reduce",
    )(dy, gate, up, w_gate, w_up, w_down)


def place_copies(n, hop, pieces, dx, bufs, in_sem, out_sem):
    me = lax.axis_index("tp")
    shards = (lax.rem(me + n - hop, n), lax.rem(me + 2 + hop, n))
    rows, half = pieces[0].shape
    ins, outs = [], []
    for way in range(2):
        at = (pl.ds(shards[way] * rows, rows), pl.ds(way * half, half))
        ins.append(pltpu.make_async_copy(pieces[way], bufs.at[way], in_sem.at[way]))
        outs.append(pltpu.make_async_copy(bufs.at[way], dx.at[at], out_sem.at[way]))
    return ins, outs


def weight_kernel(n, hop, a, b, *rest):
    pieces, rest = rest[:2], rest[-12:]
    out, dx, av, bv, ov, acc, bufs, first_sem, b_sem, o_sem, in_sem, out_sem = rest
    depth, height, cols = av.shape[0], av.shape[1] // 2, ov.shape[2]
    chunk = depth // FIRST
    blocks = bv.shape[1] // cols
    ins, outs = place_copies(n, hop, pieces, dx, bufs, in_sem, out_sem)

    def first_copies(k):
        row = pl.ds(k * chunk, chunk)
        ha, hb = (row, pl.ds(0, height)), (row, pl.ds(0, cols))
        return (
            pltpu.make_async_copy(a.at[ha], av.at[ha], first_sem.at[0, k]),
            pltpu.make_async_copy(b.at[hb], bv.at[hb], first_sem.at[1, k]),
        )

    def b_copy(j):
        at = (slice(None), pl.ds(pl.multiple_of(j * cols, cols), cols))
        return pltpu.make_async_copy(b.at[at], bv.at[at], b_sem.at[j])

    def a_copy():
        at = (slice(None), pl.ds(height, height))
        return pltpu.make_async_copy(a.at[at], av.at[at], b_sem.at[0])

    def out_copy(block):
        i, j = block // blocks, lax.rem(block, blocks)
        at = (pl.ds(pl.multiple_of(i * height, height), height), pl.ds(pl.multiple_of(j * cols, cols), cols))
        slot = lax.rem(block, 2)
        return pltpu.make_async_copy(ov.at[slot], out.at[at], o_sem.at[slot])

    for k in range(2):
        for c in first_copies(k):
            c.start()
    for k in range(FIRST):
        for c in first_copies(k):
            c.wait()
        if k + 2 < FIRST:
            for c in first_copies(k + 2):
                c.start()
        elif k + 2 == FIRST:
            for j in range(1, blocks):
                b_copy(j).start()
        else:
            a_copy().start()
            for c in ins:
                c.start()
        row = pl.ds(k * chunk, chunk)
        part = dot(av[row, pl.ds(0, height)], bv[row, pl.ds(0, cols)], TN)
        if k == 0:
            acc[...] = part
        elif k + 1 < FIRST:
            acc[...] += part
        else:
            ov[0] = (acc[...] + part).astype(BF16)
    out_copy(0).start()

    def step(block, carry):
        i, j = block // blocks, lax.rem(block, blocks)

        @pl.when(block < blocks)
        def _():
            b_copy(j).wait()

        @pl.when(block == blocks)
        def _():
            a_copy().wait()
            for c in ins:
                c.wait()
            for c in outs:
                c.start()

        @pl.when(block >= 2)
        def _():
            out_copy(block - 2).wait()

        ha = pl.ds(pl.multiple_of(i * height, height), height)
        hb = pl.ds(pl.multiple_of(j * cols, cols), cols)
        ov[lax.rem(block, 2)] = dot(av[:, ha], bv[:, hb], TN).astype(BF16)
        out_copy(block).start()
        return carry

    lax.fori_loop(1, 2 * blocks, step, 0)
    for block in (2 * blocks - 2, 2 * blocks - 1):
        out_copy(block).wait()
    for c in outs:
        c.wait()


def weight_gradient(n, hop, a, b, pieces, dx, name):
    tokens, rows, cols = a.shape[0], a.shape[1], b.shape[1]
    anywhere = pl.BlockSpec(memory_space=pltpu.MemorySpace.HBM)
    whole = (tokens, 2 * pieces[0].shape[1])
    args = (a, b, *pieces) + (() if dx is None else (dx,))
    dma = pltpu.SemaphoreType.DMA
    return pl.pallas_call(
        functools.partial(weight_kernel, n, hop),
        out_shape=(jax.ShapeDtypeStruct((rows, cols), BF16), jax.ShapeDtypeStruct(whole, BF16)),
        in_specs=[anywhere] * len(args),
        out_specs=[anywhere] * 2,
        scratch_shapes=[
            pltpu.VMEM((tokens, rows), BF16),
            pltpu.VMEM((tokens, cols), BF16),
            pltpu.VMEM((2, rows // 2, WIDE), BF16),
            pltpu.VMEM((rows // 2, WIDE), F32),
            pltpu.VMEM((2, *pieces[0].shape), BF16),
            dma((2, FIRST)),
            dma((cols // WIDE,)),
            dma((2,)),
            dma((2,)),
            dma((2,)),
        ],
        input_output_aliases={} if dx is None else {4: 1},
        compiler_params=pltpu.CompilerParams(vmem_limit_bytes=VMEM_LIMIT),
        cost_estimate=pl.CostEstimate(
            flops=2 * tokens * rows * cols, bytes_accessed=32 << 20, transcendentals=0
        ),
        name=name,
    )(*args)


def finish_kernel(n, hop, a, b, _, dx, bufs, in_sem, out_sem):
    ins, outs = place_copies(n, hop, (a, b), dx, bufs, in_sem, out_sem)
    for c in ins:
        c.start()
    for i, o in zip(ins, outs):
        i.wait()
        o.start()
    for c in outs:
        c.wait()


def finish(n, hop, pieces, dx):
    anywhere = pl.BlockSpec(memory_space=pltpu.MemorySpace.HBM)
    return pl.pallas_call(
        functools.partial(finish_kernel, n, hop),
        out_shape=jax.ShapeDtypeStruct(dx.shape, BF16),
        in_specs=[anywhere] * 3,
        out_specs=anywhere,
        scratch_shapes=[
            pltpu.VMEM((2, *pieces[0].shape), BF16),
            pltpu.SemaphoreType.DMA((2,)),
            pltpu.SemaphoreType.DMA((2,)),
        ],
        input_output_aliases={2: 0},
        compiler_params=pltpu.CompilerParams(vmem_limit_bytes=VMEM_LIMIT),
        name="finish",
    )(*pieces, dx)


def solution(mesh):
    n = mesh.shape["tp"]
    to_right = [(i, (i + 1) % n) for i in range(n)]
    to_left = [(i, (i - 1) % n) for i in range(n)]

    def step(x, dy, gate, up, w_gate, w_up, w_down):
        d_gate, d_up, hidden, *pieces = reduce_scatter(n, dy, gate, up, w_gate, w_up, w_down)
        dx, grads = None, []
        for hop, (a, b) in enumerate(((x, d_gate), (x, d_up), (hidden, dy))):
            onward = [lax.ppermute(p, "tp", ways) for p, ways in zip(pieces, (to_right, to_left))]
            grad, dx = weight_gradient(n, hop, a, b, pieces, dx, f"weight{hop}")
            grads.append(grad)
            pieces = onward
        dx = finish(n, n - 1, pieces, dx)
        return dx, *grads

    tokens, columns, rows = P("dp", None), P(None, "tp"), P("tp", None)
    return jax.shard_map(
        step,
        mesh=mesh,
        in_specs=(tokens, tokens, P("dp", "tp"), P("dp", "tp"), columns, columns, rows),
        out_specs=(tokens, P("dp", "tp"), P("dp", "tp"), P(("dp", "tp"), None)),
        check_vma=False,
    )
```

```python
import functools

import jax
import jax.numpy as jnp
from jax import lax
from jax.experimental import pallas as pl
from jax.experimental.pallas import tpu as pltpu
from jax.sharding import PartitionSpec as P


BF16, F32 = jnp.bfloat16, jnp.float32
NT = (((1,), (1,)), ((), ()))
TN = (((0,), (0,)), ((), ()))
TILE = 512
STRIP = 16
WIDE = 512
FIRST = 2
CUTS = 4
EARLY = 4
VMEM_LIMIT = 67043328


def dot(a, b, dims):
    return lax.dot_general(a, b, dims, preferred_element_type=F32)


def reduce_kernel(
    n, dy, gate, up, w_gate, w_up, w_down,
    d_gate, d_up, hidden, sum_a, sum_b, next_a, next_b, d_down,
    wd, wgu, dgu, dyb, gb, ub, acc_a, acc_b, first, recv, own, ahead,
    wd_sem, wgu_sem, dy_sem, g_sem, u_sem, h_sem, out_sem, fin_sem, send_sem, recv_sem, load_sem, down_sem, ag_sem, ag_recv_sem, next_sem,
):
    rows, width = dyb.shape[1], wd.shape[1]
    half_rows = rows // 2
    units = wd.shape[0]
    tiles = units // TILE
    pieces = width // 2 // TILE
    me = lax.axis_index("tp")
    right, left = lax.rem(me + 1, n), lax.rem(me + n - 1, n)
    places = ((0, 0), (1, 2), (0, 0), (2, 1))

    def half(h):
        return pl.ds(pl.multiple_of(h * half_rows, half_rows), half_rows)

    def rows_of(k, h):
        shard = lax.rem(me + (3, 2, 0, 1)[k], n) if isinstance(k, int) else lax.rem(me + n - 2 * k, n)
        return pl.ds(pl.multiple_of(shard * rows + h * half_rows, half_rows), half_rows)

    def tile_at(t):
        return pl.ds(pl.multiple_of(t * TILE, TILE), TILE)

    def dy_copy(k, h):
        side = lax.rem(k, 2)
        return pltpu.make_async_copy(dy.at[rows_of(k, h), :], dyb.at[side, half(h), :], dy_sem.at[side, h])

    def act_copies(k, h, t):
        side, at = lax.rem(k, 2), tile_at(t)
        return (
            pltpu.make_async_copy(gate.at[rows_of(k, h), at], gb.at[side, half(h), at], g_sem.at[side, h, t]),
            pltpu.make_async_copy(up.at[rows_of(k, h), at], ub.at[side, half(h), at], u_sem.at[side, h, t]),
        )

    def fetch(k, h):
        dy_copy(k, h).start()
        for t in range(tiles):
            for c in act_copies(k, h, t):
                c.start()

    def hidden_copy(k, h):
        side = lax.rem(k, 2)
        return pltpu.make_async_copy(gb.at[side, half(h), :], hidden.at[rows_of(k, h), :], h_sem.at[side, h])

    def out_copies(k, h):
        slot = lax.rem(k, n - 1)
        return tuple(
            pltpu.make_async_copy(
                dgu.at[slot, half(h), pl.ds(i * units, units)], out.at[rows_of(k, h), :], out_sem.at[i, slot, h]
            )
            for i, out in enumerate((d_gate, d_up))
        )

    def flush(k, h):
        hidden_copy(k, h).start()
        for c in out_copies(k, h):
            c.start()

    def wd_copy(t):
        at = tile_at(t)
        return pltpu.make_async_copy(w_down.at[at, :], wd.at[at, :], wd_sem.at[t])

    def wgu_copies(q):
        c = lax.rem(q, 2) * pieces + q // 2
        at = tile_at(c)
        return (
            pltpu.make_async_copy(w_gate.at[at, :], wgu.at[at, pl.ds(0, units)], wgu_sem.at[0, c]),
            pltpu.make_async_copy(w_up.at[at, :], wgu.at[at, pl.ds(units, units)], wgu_sem.at[1, c]),
        )

    def weights(q):
        for c in wgu_copies(q):
            c.start()

    def remote(src, hop, way, m):
        return pltpu.make_async_remote_copy(
            src_ref=src,
            dst_ref=recv.at[way, hop, m],
            send_sem=send_sem.at[way, hop, m],
            recv_sem=recv_sem.at[way, hop, m],
            device_id={"tp": lax.rem(me + 1 + way * (n - 2), n)},
            device_id_type=pl.DeviceIdType.MESH,
        )

    dy_copy(0, 0).start()
    for t in range(2):
        wd_copy(t).start()
    for c in act_copies(0, 0, 0):
        c.start()

    barrier = pltpu.get_barrier_semaphore()
    for other in (left, right):
        pl.semaphore_signal(barrier, inc=1, device_id={"tp": other}, device_id_type=pl.DeviceIdType.MESH)

    def gradients(k, h):
        side, slot = lax.rem(k, 2), lax.rem(k, n - 1)
        opening = isinstance(k, int) and k == 0
        accs = (acc_a, acc_b)

        def product(t):
            accs[t % 2][...] = dot(dyb[side, half(h), :], wd[t * TILE : (t + 1) * TILE, :], NT)

        def finish(t):
            cols, more = pl.ds(t * TILE, TILE), pl.ds(units + t * TILE, TILE)
            for r in range(0, half_rows, STRIP):
                row = pl.ds(pl.multiple_of(h * half_rows + r, STRIP), STRIP)
                g = gb[side, row, cols].astype(F32)
                u = ub[side, row, cols].astype(F32)
                d_hidden = accs[t % 2][r : r + STRIP, :]
                sig = 1.0 / (1.0 + jnp.exp(-g))
                silu = g * sig
                gb[side, row, cols] = (silu * u).astype(BF16)
                dgu[slot, row, cols] = (d_hidden * u * (sig + silu * (1.0 - sig))).astype(BF16)
                dgu[slot, row, more] = (d_hidden * silu).astype(BF16)

        def arrive(t):
            @pl.when(h == 0)
            def _():
                wd_copy(t).wait()
                if t + 2 < tiles:
                    wd_copy(t + 2).start()
                else:
                    weights(t + 2 - tiles)
                if t + 1 < tiles:
                    for c in act_copies(k, 0, t + 1):
                        c.start()

        def ready(t):
            for c in act_copies(k, h, t):
                c.wait()

        dy_copy(k, h).wait()
        if not opening:
            for t in range(tiles):
                ready(t)
        for t in range(tiles):
            if opening:
                arrive(t)
                if t > 0:
                    ready(t - 1)
            product(t)
            if t > 0:
                finish(t - 1)
        if opening:
            ready(tiles - 1)
        finish(tiles - 1)

    def term(hop, way, h, c, out):
        a, b = places[hop]
        at = pl.ds(pl.multiple_of((way * pieces + c) * TILE, TILE), TILE)
        out[...] = dot(dgu[a + way * (b - a), half(h), :], wgu[at, :], NT)

    def round_to(ref, mine, old=None):
        for r in range(0, half_rows, STRIP):
            row = pl.ds(r, STRIP)
            value = mine[row, :]
            if old is not None:
                value = value + old[row, :].astype(F32)
            ref[row, :] = value.astype(BF16)

    def later(hop, way, h, c):
        m = h * pieces + c
        here = recv.at[way, hop - 1, m]
        term(hop, way, h, c, acc_a)
        remote(here, hop - 1, way, m).wait_recv()
        round_to(here, acc_a, here)
        remote(here, hop, way, m).start()

    def hop0(h, carry):
        gradients(0, h)

        @pl.when(h == 0)
        def _():
            for q in range(2, 2 * pieces):
                weights(q)
            fetch(0, 1)
            pl.semaphore_wait(barrier, 2)

        @pl.when(h == 1)
        def _():
            fetch(1, 0)
            fetch(1, 1)

        def message(q, carry):
            way, c = lax.rem(q, 2), q // 2

            @pl.when(h == 0)
            def _():
                for copy in wgu_copies(q):
                    copy.wait()

            m = h * pieces + c
            term(0, way, h, c, acc_a)
            round_to(first.at[way, m], acc_a)
            remote(first.at[way, m], 0, way, m).start()
            return carry

        lax.fori_loop(0, 2 * pieces, message, 0)
        flush(0, h)
        return carry

    lax.fori_loop(0, 2, hop0, 0)
    for h in range(2):
        hidden_copy(0, h).wait()
        fetch(2, h)

    def hop1(h, carry):
        def shard(k, carry):
            gradients(k, h)

            def message(c, carry):
                later(1, k - 1, h, c)
                return carry

            lax.fori_loop(0, pieces, message, 0)
            flush(k, h)
            return carry

        lax.fori_loop(1, n - 1, shard, 0)
        hidden_copy(1, h).wait()
        fetch(3, h)
        return carry

    lax.fori_loop(0, 2, hop1, 0)
    for h in range(2):
        for c in out_copies(0, h):
            c.wait()

    def hop2(h, carry):
        gradients(3, h)

        def message(q, carry):
            later(2, lax.rem(q, 2), h, q // 2)
            return carry

        lax.fori_loop(0, 2 * pieces, message, 0)
        flush(3, h)
        return carry

    lax.fori_loop(0, 2, hop2, 0)

    order = (2, 3, 0, 1)

    def down_loads():
        loads = []
        for i, k in enumerate(order):
            shard = pl.ds(pl.multiple_of(lax.rem(me + (3, 2, 0, 1)[k], n) * rows, rows), rows)
            loads.append(pltpu.make_async_copy(dy.at[shard, :], wd.at[pl.ds(i * rows, rows), :], load_sem.at[i]))
            if k < 2:
                loads.append(pltpu.make_async_copy(hidden.at[shard, :], ub.at[k], load_sem.at[n + k]))
        return loads

    def down_copy(m):
        slab = dyb.at[lax.rem(m, 4) // 2, half(lax.rem(m, 2)), :]
        at = pl.ds(pl.multiple_of(m * half_rows, half_rows), half_rows)
        return pltpu.make_async_copy(slab, d_down.at[at, :], down_sem.at[lax.rem(m, 4)])

    down_tiles = width // TILE
    down_blocks = units // half_rows * down_tiles

    def down(block, carry):
        m, j = block // down_tiles, lax.rem(block, down_tiles)

        @pl.when(jnp.logical_and(j == 0, m >= 4))
        def _():
            down_copy(m - 4).wait()

        at = pl.ds(pl.multiple_of(m * half_rows, half_rows), half_rows)
        total = None
        for i, src in enumerate((gb.at[0], gb.at[1], ub.at[0], ub.at[1])):
            part = dot(src[:, at], wd[i * rows : (i + 1) * rows, tile_at(j)], TN)
            total = part if total is None else total + part
        dyb[lax.rem(m, 4) // 2, half(lax.rem(m, 2)), tile_at(j)] = total.astype(BF16)

        @pl.when(j == down_tiles - 1)
        def _():
            down_copy(m).start()

        return carry

    def onward(way, m):
        return pltpu.make_async_remote_copy(
            src_ref=recv.at[way, n - 2, m],
            dst_ref=ahead.at[way, m],
            send_sem=ag_sem.at[way, m],
            recv_sem=ag_recv_sem.at[way, m],
            device_id={"tp": lax.rem(me + 1 + way * (n - 2), n)},
            device_id_type=pl.DeviceIdType.MESH,
        )

    def final_copy(way, h, c):
        out = (sum_a, sum_b)[way]
        m = h * pieces + c
        return pltpu.make_async_copy(
            recv.at[way, n - 2, m], out.at[half(h), tile_at(c)], fin_sem.at[way, m]
        )

    def next_copy(way, h, c):
        out = (next_a, next_b)[way]
        m = h * pieces + c
        return pltpu.make_async_copy(ahead.at[way, m], out.at[half(h), tile_at(c)], next_sem.at[way, m])

    def close(way, h, c, mine):
        m = h * pieces + c
        last = recv.at[way, n - 2, m]
        remote(last, n - 2, way, m).wait_recv()
        round_to(last, mine, last)
        onward(way, m).start()
        final_copy(way, h, c).start()

    for c in down_loads():
        c.start()

    def keep(q, carry):
        way, c = lax.rem(q, 2), q // 2
        term(n - 1, way, 1, c, own.at[way, c])
        return carry

    lax.fori_loop(0, 2 * pieces, keep, 0)

    def early(c, carry):
        for way in range(2):
            term(n - 1, way, 0, c, acc_a)
            close(way, 0, c, acc_a)
        return carry

    lax.fori_loop(0, pieces, early, 0)
    for c in down_loads():
        c.wait()

    def late(c, carry):
        lax.fori_loop(c * EARLY, (c + 1) * EARLY, down, 0)
        for way in range(2):
            close(way, 1, c, own.at[way, c])
        return carry

    lax.fori_loop(0, pieces, late, 0)
    lax.fori_loop(pieces * EARLY, down_blocks, down, 0)
    for m in range(units // half_rows - 4, units // half_rows):
        down_copy(m).wait()
    for h in range(2):
        for k in (n - 2, n - 1):
            hidden_copy(k, h).wait()
        for k in range(1, n):
            for c in out_copies(k, h):
                c.wait()
        for c in range(pieces):
            m = h * pieces + c
            for way in range(2):
                remote(first.at[way, m], 0, way, m).wait_send()
                for hop in range(1, n - 1):
                    remote(recv.at[way, hop - 1, m], hop, way, m).wait_send()
                final_copy(way, h, c).wait()
    for h in range(2):
        for c in range(pieces):
            for way in range(2):
                onward(way, h * pieces + c).wait_recv()
                next_copy(way, h, c).start()
    for h in range(2):
        for c in range(pieces):
            for way in range(2):
                onward(way, h * pieces + c).wait_send()
                next_copy(way, h, c).wait()


def reduce_scatter(n, dy, gate, up, w_gate, w_up, w_down):
    tokens, width = dy.shape
    units = gate.shape[1]
    rows, half = tokens // n, width // 2
    pieces = half // TILE
    block = (rows // 2, TILE)
    wide = jax.ShapeDtypeStruct((tokens, units), BF16)
    part = jax.ShapeDtypeStruct((rows, half), BF16)
    dma = pltpu.SemaphoreType.DMA
    return pl.pallas_call(
        functools.partial(reduce_kernel, n),
        out_shape=(wide, wide, wide, part, part, part, part, jax.ShapeDtypeStruct((units, width), BF16)),
        in_specs=[pl.BlockSpec(memory_space=pltpu.MemorySpace.HBM)] * 6,
        out_specs=[pl.BlockSpec(memory_space=pltpu.MemorySpace.HBM)] * 8,
        scratch_shapes=[
            pltpu.VMEM((units, width), BF16),
            pltpu.VMEM((width, 2 * units), BF16),
            pltpu.VMEM((n - 1, rows, 2 * units), BF16),
            pltpu.VMEM((2, rows, width), BF16),
            pltpu.VMEM((2, rows, units), BF16),
            pltpu.VMEM((2, rows, units), BF16),
            pltpu.VMEM(block, F32),
            pltpu.VMEM(block, F32),
            pltpu.VMEM((2, 2 * pieces, *block), BF16),
            pltpu.VMEM((2, n - 1, 2 * pieces, *block), BF16),
            pltpu.VMEM((2, pieces, *block), F32),
            pltpu.VMEM((2, 2 * pieces, *block), BF16),
            dma((units // TILE,)),
            dma((2, width // TILE)),
            dma((2, 2)),
            dma((2, 2, units // TILE)),
            dma((2, 2, units // TILE)),
            dma((2, 2)),
            dma((2, n - 1, 2)),
            dma((2, 2 * pieces)),
            dma((2, n - 1, 2 * pieces)),
            dma((2, n - 1, 2 * pieces)),
            dma((n + 2,)),
            dma((4,)),
            dma((2, 2 * pieces)),
            dma((2, 2 * pieces)),
            dma((2, 2 * pieces)),
        ],
        compiler_params=pltpu.CompilerParams(
            collective_id=0, has_side_effects=True, vmem_limit_bytes=VMEM_LIMIT
        ),
        cost_estimate=pl.CostEstimate(
            flops=8 * tokens * width * units, bytes_accessed=96 << 20, transcendentals=0
        ),
        name="reduce",
    )(dy, gate, up, w_gate, w_up, w_down)


def place_copies(n, hop, pieces, dx, bufs, in_sem, out_sem):
    me = lax.axis_index("tp")
    shards = (lax.rem(me + n - hop, n), lax.rem(me + 2 + hop, n))
    rows, half = pieces[0].shape
    ins, outs = [], []
    for way in range(2):
        at = (pl.ds(shards[way] * rows, rows), pl.ds(way * half, half))
        ins.append(pltpu.make_async_copy(pieces[way], bufs.at[way], in_sem.at[way]))
        outs.append(pltpu.make_async_copy(bufs.at[way], dx.at[at], out_sem.at[way]))
    return ins, outs


def weight_kernel(n, hops, a, b, down, *rest):
    pieces, rest = rest[: 2 * len(hops)], rest[-15:]
    out, dx, d_down, av, bv, ov, acc, bufs, dbuf, first_sem, b_sem, o_sem, in_sem, out_sem, d_sem = rest
    depth, height, cols = av.shape[0], av.shape[1] // 2, ov.shape[2]
    chunk = depth // FIRST
    blocks = bv.shape[1] // cols
    ins, outs = [], []
    for i, hop in enumerate(hops):
        two = place_copies(n, hop, pieces[2 * i : 2 * i + 2], dx, bufs.at[i], in_sem.at[i], out_sem.at[i])
        ins, outs = ins + two[0], outs + two[1]
    at = pl.ds((hops[0] // 2) * dbuf.shape[0], dbuf.shape[0])
    ins.append(pltpu.make_async_copy(down.at[at, :], dbuf, d_sem.at[0]))
    outs.append(pltpu.make_async_copy(dbuf, d_down.at[at, :], d_sem.at[1]))

    def first_copies(k):
        row = pl.ds(k * chunk, chunk)
        ha, hb = (row, pl.ds(0, height)), (row, pl.ds(0, cols))
        return (
            pltpu.make_async_copy(a.at[ha], av.at[ha], first_sem.at[0, k]),
            pltpu.make_async_copy(b.at[hb], bv.at[hb], first_sem.at[1, k]),
        )

    def b_copy(j):
        at = (slice(None), pl.ds(pl.multiple_of(j * cols, cols), cols))
        return pltpu.make_async_copy(b.at[at], bv.at[at], b_sem.at[j])

    def a_copy():
        at = (slice(None), pl.ds(height, height))
        return pltpu.make_async_copy(a.at[at], av.at[at], b_sem.at[0])

    def out_copy(block):
        i, j = block // blocks, lax.rem(block, blocks)
        at = (pl.ds(pl.multiple_of(i * height, height), height), pl.ds(pl.multiple_of(j * cols, cols), cols))
        slot = lax.rem(block, 2)
        return pltpu.make_async_copy(ov.at[slot], out.at[at], o_sem.at[slot])

    for k in range(2):
        for c in first_copies(k):
            c.start()
    for k in range(FIRST):
        for c in first_copies(k):
            c.wait()
        if k + 2 < FIRST:
            for c in first_copies(k + 2):
                c.start()
        elif k + 2 == FIRST:
            for j in range(1, blocks):
                b_copy(j).start()
        else:
            a_copy().start()
            for c in ins:
                c.start()
        row = pl.ds(k * chunk, chunk)
        part = dot(av[row, pl.ds(0, height)], bv[row, pl.ds(0, cols)], TN)
        if k == 0:
            acc[...] = part
        elif k + 1 < FIRST:
            acc[...] += part
        else:
            ov[0] = (acc[...] + part).astype(BF16)
    out_copy(0).start()

    def step(block, carry):
        i, j = block // blocks, lax.rem(block, blocks)

        @pl.when(block < blocks)
        def _():
            b_copy(j).wait()

        @pl.when(block == blocks)
        def _():
            a_copy().wait()
            for c in ins:
                c.wait()
            for c in outs:
                c.start()

        @pl.when(block >= 2)
        def _():
            out_copy(block - 2).wait()

        ha = pl.ds(pl.multiple_of(i * height, height), height)
        hb = pl.ds(pl.multiple_of(j * cols, cols), cols)
        ov[lax.rem(block, 2)] = dot(av[:, ha], bv[:, hb], TN).astype(BF16)
        out_copy(block).start()
        return carry

    lax.fori_loop(1, 2 * blocks, step, 0)
    for block in (2 * blocks - 2, 2 * blocks - 1):
        out_copy(block).wait()
    for c in outs:
        c.wait()


def weight_gradient(n, hops, a, b, down, pieces, old, name):
    tokens, rows, cols = a.shape[0], a.shape[1], b.shape[1]
    anywhere = pl.BlockSpec(memory_space=pltpu.MemorySpace.HBM)
    shapes = ((rows, cols), (tokens, 2 * pieces[0].shape[1]), down.shape)
    args = (a, b, down, *pieces, *old)
    dma = pltpu.SemaphoreType.DMA
    return pl.pallas_call(
        functools.partial(weight_kernel, n, hops),
        out_shape=tuple(jax.ShapeDtypeStruct(shape, BF16) for shape in shapes),
        in_specs=[anywhere] * len(args),
        out_specs=[anywhere] * 3,
        scratch_shapes=[
            pltpu.VMEM((tokens, rows), BF16),
            pltpu.VMEM((tokens, cols), BF16),
            pltpu.VMEM((2, rows // 2, WIDE), BF16),
            pltpu.VMEM((rows // 2, WIDE), F32),
            pltpu.VMEM((len(hops), 2, *pieces[0].shape), BF16),
            pltpu.VMEM((down.shape[0] // 2, down.shape[1]), BF16),
            dma((2, FIRST)),
            dma((cols // WIDE,)),
            dma((2,)),
            dma((len(hops), 2)),
            dma((len(hops), 2)),
            dma((2,)),
        ],
        input_output_aliases={len(args) - 2 + i: 1 + i for i in range(len(old))},
        compiler_params=pltpu.CompilerParams(vmem_limit_bytes=VMEM_LIMIT),
        cost_estimate=pl.CostEstimate(
            flops=2 * tokens * rows * cols, bytes_accessed=48 << 20, transcendentals=0
        ),
        name=name,
    )(*args)


def finish_kernel(n, hop, a, b, _, dx, bufs, in_sem, out_sem):
    me = lax.axis_index("tp")
    shards = (lax.rem(me + n - hop, n), lax.rem(me + 2 + hop, n))
    rows, half = a.shape
    size = rows // CUTS
    ins, outs = [], []
    for cut in range(CUTS):
        for way, piece in enumerate((a, b)):
            here = pl.ds(cut * size, size)
            there = (pl.ds(shards[way] * rows + cut * size, size), pl.ds(way * half, half))
            buf = bufs.at[way, here, :]
            ins.append(pltpu.make_async_copy(piece.at[here, :], buf, in_sem.at[way, cut]))
            outs.append(pltpu.make_async_copy(buf, dx.at[there], out_sem.at[way, cut]))
    for c in ins:
        c.start()
    for i, o in zip(ins, outs):
        i.wait()
        o.start()
    for c in outs:
        c.wait()


def finish(n, hop, pieces, dx):
    anywhere = pl.BlockSpec(memory_space=pltpu.MemorySpace.HBM)
    return pl.pallas_call(
        functools.partial(finish_kernel, n, hop),
        out_shape=jax.ShapeDtypeStruct(dx.shape, BF16),
        in_specs=[anywhere] * 3,
        out_specs=anywhere,
        scratch_shapes=[
            pltpu.VMEM((2, *pieces[0].shape), BF16),
            pltpu.SemaphoreType.DMA((2, CUTS)),
            pltpu.SemaphoreType.DMA((2, CUTS)),
        ],
        input_output_aliases={2: 0},
        compiler_params=pltpu.CompilerParams(vmem_limit_bytes=VMEM_LIMIT),
        name="finish",
    )(*pieces, dx)


def solution(mesh):
    n = mesh.shape["tp"]
    to_right = [(i, (i + 1) % n) for i in range(n)]
    to_left = [(i, (i - 1) % n) for i in range(n)]

    def step(x, dy, gate, up, w_gate, w_up, w_down):
        d_gate, d_up, _, *parts, down = reduce_scatter(n, dy, gate, up, w_gate, w_up, w_down)
        own, pieces = parts[:2], parts[2:]

        def onward(pieces):
            return [lax.ppermute(p, "tp", ways) for p, ways in zip(pieces, (to_right, to_left))]

        later = onward(pieces)
        dw_gate, *old = weight_gradient(n, (0, 1), x, d_gate, down, (*own, *pieces), (), "weight0")
        last = onward(later)
        dw_up, dx, dw_down = weight_gradient(n, (2,), x, d_up, down, later, old, "weight1")
        return finish(n, n - 1, last, dx), dw_gate, dw_up, dw_down

    tokens, columns, rows = P("dp", None), P(None, "tp"), P("tp", None)
    return jax.shard_map(
        step,
        mesh=mesh,
        in_specs=(tokens, tokens, P("dp", "tp"), P("dp", "tp"), columns, columns, rows),
        out_specs=(tokens, P("dp", "tp"), P("dp", "tp"), P(("dp", "tp"), None)),
        check_vma=False,
    )
```

```python
import functools

import jax
import jax.numpy as jnp
from jax import lax
from jax.experimental import pallas as pl
from jax.experimental.pallas import tpu as pltpu
from jax.sharding import PartitionSpec as P


BF16, F32 = jnp.bfloat16, jnp.float32
NT = (((1,), (1,)), ((), ()))
TN = (((0,), (0,)), ((), ()))
TILE = 512
STRIP = 16
WIDE = 512
FIRST = 2
EARLY = 4
VMEM_LIMIT = 67043328


def dot(a, b, dims):
    return lax.dot_general(a, b, dims, preferred_element_type=F32)


def reduce_kernel(
    n, dy, gate, up, w_gate, w_up, w_down,
    d_gate, d_up, hidden, sum_a, sum_b, next_a, next_b, d_down,
    wd, wgu, dgu, dyb, gb, ub, acc_a, acc_b, first, recv, own, ahead,
    wd_sem, wgu_sem, dy_sem, g_sem, u_sem, h_sem, out_sem, fin_sem, send_sem, recv_sem, load_sem, down_sem, ag_sem, ag_recv_sem, next_sem,
):
    rows, width = dyb.shape[1], wd.shape[1]
    half_rows = rows // 2
    units = wd.shape[0]
    tiles = units // TILE
    pieces = width // 2 // TILE
    me = lax.axis_index("tp")
    right, left = lax.rem(me + 1, n), lax.rem(me + n - 1, n)
    places = ((0, 0), (1, 2), (0, 0), (2, 1))

    def half(h):
        return pl.ds(pl.multiple_of(h * half_rows, half_rows), half_rows)

    def rows_of(k, h):
        shard = lax.rem(me + (3, 2, 0, 1)[k], n) if isinstance(k, int) else lax.rem(me + n - 2 * k, n)
        return pl.ds(pl.multiple_of(shard * rows + h * half_rows, half_rows), half_rows)

    def tile_at(t):
        return pl.ds(pl.multiple_of(t * TILE, TILE), TILE)

    def dy_copy(k, h):
        side = lax.rem(k, 2)
        return pltpu.make_async_copy(dy.at[rows_of(k, h), :], dyb.at[side, half(h), :], dy_sem.at[side, h])

    def act_copies(k, h, t):
        side, at = lax.rem(k, 2), tile_at(t)
        return (
            pltpu.make_async_copy(gate.at[rows_of(k, h), at], gb.at[side, half(h), at], g_sem.at[side, h, t]),
            pltpu.make_async_copy(up.at[rows_of(k, h), at], ub.at[side, half(h), at], u_sem.at[side, h, t]),
        )

    def fetch(k, h):
        dy_copy(k, h).start()
        for t in range(tiles):
            for c in act_copies(k, h, t):
                c.start()

    def hidden_copy(k, h):
        side = lax.rem(k, 2)
        return pltpu.make_async_copy(gb.at[side, half(h), :], hidden.at[rows_of(k, h), :], h_sem.at[side, h])

    def out_copies(k, h):
        slot = lax.rem(k, n - 1)
        return tuple(
            pltpu.make_async_copy(
                dgu.at[slot, half(h), pl.ds(i * units, units)], out.at[rows_of(k, h), :], out_sem.at[i, slot, h]
            )
            for i, out in enumerate((d_gate, d_up))
        )

    def flush(k, h):
        hidden_copy(k, h).start()
        for c in out_copies(k, h):
            c.start()

    def wd_copy(t):
        at = tile_at(t)
        return pltpu.make_async_copy(w_down.at[at, :], wd.at[at, :], wd_sem.at[t])

    def wgu_copies(q):
        c = lax.rem(q, 2) * pieces + q // 2
        at = tile_at(c)
        return (
            pltpu.make_async_copy(w_gate.at[at, :], wgu.at[at, pl.ds(0, units)], wgu_sem.at[0, c]),
            pltpu.make_async_copy(w_up.at[at, :], wgu.at[at, pl.ds(units, units)], wgu_sem.at[1, c]),
        )

    def weights(q):
        for c in wgu_copies(q):
            c.start()

    def remote(src, hop, way, m):
        return pltpu.make_async_remote_copy(
            src_ref=src,
            dst_ref=recv.at[way, hop, m],
            send_sem=send_sem.at[way, hop, m],
            recv_sem=recv_sem.at[way, hop, m],
            device_id={"tp": lax.rem(me + 1 + way * (n - 2), n)},
            device_id_type=pl.DeviceIdType.MESH,
        )

    dy_copy(0, 0).start()
    for t in range(2):
        wd_copy(t).start()
    for c in act_copies(0, 0, 0):
        c.start()

    barrier = pltpu.get_barrier_semaphore()
    for other in (left, right):
        pl.semaphore_signal(barrier, inc=1, device_id={"tp": other}, device_id_type=pl.DeviceIdType.MESH)

    def gradients(k, h):
        side, slot = lax.rem(k, 2), lax.rem(k, n - 1)
        opening = isinstance(k, int) and k == 0
        accs = (acc_a, acc_b)

        def product(t):
            accs[t % 2][...] = dot(dyb[side, half(h), :], wd[t * TILE : (t + 1) * TILE, :], NT)

        def finish(t):
            cols, more = pl.ds(t * TILE, TILE), pl.ds(units + t * TILE, TILE)
            for r in range(0, half_rows, STRIP):
                row = pl.ds(pl.multiple_of(h * half_rows + r, STRIP), STRIP)
                g = gb[side, row, cols].astype(F32)
                u = ub[side, row, cols].astype(F32)
                d_hidden = accs[t % 2][r : r + STRIP, :]
                sig = 1.0 / (1.0 + jnp.exp(-g))
                silu = g * sig
                gb[side, row, cols] = (silu * u).astype(BF16)
                dgu[slot, row, cols] = (d_hidden * u * (sig + silu * (1.0 - sig))).astype(BF16)
                dgu[slot, row, more] = (d_hidden * silu).astype(BF16)

        def arrive(t):
            @pl.when(h == 0)
            def _():
                wd_copy(t).wait()
                if t + 2 < tiles:
                    wd_copy(t + 2).start()
                else:
                    weights(t + 2 - tiles)
                if t + 1 < tiles:
                    for c in act_copies(k, 0, t + 1):
                        c.start()

        def ready(t):
            for c in act_copies(k, h, t):
                c.wait()

        dy_copy(k, h).wait()
        if not opening:
            for t in range(tiles):
                ready(t)
        for t in range(tiles):
            if opening:
                arrive(t)
                if t > 0:
                    ready(t - 1)
            product(t)
            if t > 0:
                finish(t - 1)
        if opening:
            ready(tiles - 1)
        finish(tiles - 1)

    def term(hop, way, h, c, out):
        a, b = places[hop]
        at = pl.ds(pl.multiple_of((way * pieces + c) * TILE, TILE), TILE)
        out[...] = dot(dgu[a + way * (b - a), half(h), :], wgu[at, :], NT)

    def round_to(ref, mine, old=None):
        for r in range(0, half_rows, STRIP):
            row = pl.ds(r, STRIP)
            value = mine[row, :]
            if old is not None:
                value = value + old[row, :].astype(F32)
            ref[row, :] = value.astype(BF16)

    def later(hop, way, h, c):
        m = h * pieces + c
        here = recv.at[way, hop - 1, m]
        term(hop, way, h, c, acc_a)
        remote(here, hop - 1, way, m).wait_recv()
        round_to(here, acc_a, here)
        remote(here, hop, way, m).start()

    def hop0(h, carry):
        gradients(0, h)

        @pl.when(h == 0)
        def _():
            for q in range(2, 2 * pieces):
                weights(q)
            fetch(0, 1)
            pl.semaphore_wait(barrier, 2)

        @pl.when(h == 1)
        def _():
            fetch(1, 0)
            fetch(1, 1)

        def message(q, carry):
            way, c = lax.rem(q, 2), q // 2

            @pl.when(h == 0)
            def _():
                for copy in wgu_copies(q):
                    copy.wait()

            m = h * pieces + c
            term(0, way, h, c, acc_a)
            round_to(first.at[way, m], acc_a)
            remote(first.at[way, m], 0, way, m).start()
            return carry

        lax.fori_loop(0, 2 * pieces, message, 0)
        flush(0, h)
        return carry

    lax.fori_loop(0, 2, hop0, 0)
    for h in range(2):
        hidden_copy(0, h).wait()
        fetch(2, h)

    def hop1(h, carry):
        def shard(k, carry):
            gradients(k, h)

            def message(c, carry):
                later(1, k - 1, h, c)
                return carry

            lax.fori_loop(0, pieces, message, 0)
            flush(k, h)
            return carry

        lax.fori_loop(1, n - 1, shard, 0)
        hidden_copy(1, h).wait()
        fetch(3, h)
        return carry

    lax.fori_loop(0, 2, hop1, 0)
    for h in range(2):
        for c in out_copies(0, h):
            c.wait()

    def hop2(h, carry):
        gradients(3, h)

        def message(q, carry):
            later(2, lax.rem(q, 2), h, q // 2)
            return carry

        lax.fori_loop(0, 2 * pieces, message, 0)
        flush(3, h)
        return carry

    lax.fori_loop(0, 2, hop2, 0)

    order = (2, 3, 0, 1)

    def down_loads():
        loads = []
        for i, k in enumerate(order):
            shard = pl.ds(pl.multiple_of(lax.rem(me + (3, 2, 0, 1)[k], n) * rows, rows), rows)
            loads.append(pltpu.make_async_copy(dy.at[shard, :], wd.at[pl.ds(i * rows, rows), :], load_sem.at[i]))
            if k < 2:
                loads.append(pltpu.make_async_copy(hidden.at[shard, :], ub.at[k], load_sem.at[n + k]))
        return loads

    def down_copy(m):
        slab = dyb.at[lax.rem(m, 4) // 2, half(lax.rem(m, 2)), :]
        at = pl.ds(pl.multiple_of(m * half_rows, half_rows), half_rows)
        return pltpu.make_async_copy(slab, d_down.at[at, :], down_sem.at[lax.rem(m, 4)])

    down_tiles = width // TILE
    down_blocks = units // half_rows * down_tiles

    def down(block, carry):
        m, j = block // down_tiles, lax.rem(block, down_tiles)

        @pl.when(jnp.logical_and(j == 0, m >= 4))
        def _():
            down_copy(m - 4).wait()

        at = pl.ds(pl.multiple_of(m * half_rows, half_rows), half_rows)
        total = None
        for i, src in enumerate((gb.at[0], gb.at[1], ub.at[0], ub.at[1])):
            part = dot(src[:, at], wd[i * rows : (i + 1) * rows, tile_at(j)], TN)
            total = part if total is None else total + part
        dyb[lax.rem(m, 4) // 2, half(lax.rem(m, 2)), tile_at(j)] = total.astype(BF16)

        @pl.when(j == down_tiles - 1)
        def _():
            down_copy(m).start()

        return carry

    def onward(way, m):
        return pltpu.make_async_remote_copy(
            src_ref=recv.at[way, n - 2, m],
            dst_ref=ahead.at[way, m],
            send_sem=ag_sem.at[way, m],
            recv_sem=ag_recv_sem.at[way, m],
            device_id={"tp": lax.rem(me + 1 + way * (n - 2), n)},
            device_id_type=pl.DeviceIdType.MESH,
        )

    def final_copy(way, h, c):
        out = (sum_a, sum_b)[way]
        m = h * pieces + c
        return pltpu.make_async_copy(
            recv.at[way, n - 2, m], out.at[half(h), tile_at(c)], fin_sem.at[way, m]
        )

    def next_copy(way, h, c):
        out = (next_a, next_b)[way]
        m = h * pieces + c
        return pltpu.make_async_copy(ahead.at[way, m], out.at[half(h), tile_at(c)], next_sem.at[way, m])

    def close(way, h, c, mine):
        m = h * pieces + c
        last = recv.at[way, n - 2, m]
        remote(last, n - 2, way, m).wait_recv()
        round_to(last, mine, last)
        onward(way, m).start()
        final_copy(way, h, c).start()

    for c in down_loads():
        c.start()

    def keep(q, carry):
        way, c = lax.rem(q, 2), q // 2
        term(n - 1, way, 1, c, own.at[way, c])
        return carry

    lax.fori_loop(0, 2 * pieces, keep, 0)

    def early(c, carry):
        for way in range(2):
            term(n - 1, way, 0, c, acc_a)
            close(way, 0, c, acc_a)
        return carry

    lax.fori_loop(0, pieces, early, 0)
    for c in down_loads():
        c.wait()

    def late(c, carry):
        lax.fori_loop(c * EARLY, (c + 1) * EARLY, down, 0)
        for way in range(2):
            close(way, 1, c, own.at[way, c])
        return carry

    lax.fori_loop(0, pieces, late, 0)
    lax.fori_loop(pieces * EARLY, down_blocks, down, 0)
    for m in range(units // half_rows - 4, units // half_rows):
        down_copy(m).wait()
    for h in range(2):
        for k in (n - 2, n - 1):
            hidden_copy(k, h).wait()
        for k in range(1, n):
            for c in out_copies(k, h):
                c.wait()
        for c in range(pieces):
            m = h * pieces + c
            for way in range(2):
                remote(first.at[way, m], 0, way, m).wait_send()
                for hop in range(1, n - 1):
                    remote(recv.at[way, hop - 1, m], hop, way, m).wait_send()
                final_copy(way, h, c).wait()
    for h in range(2):
        for c in range(pieces):
            for way in range(2):
                onward(way, h * pieces + c).wait_recv()
                next_copy(way, h, c).start()
    for h in range(2):
        for c in range(pieces):
            for way in range(2):
                onward(way, h * pieces + c).wait_send()
                next_copy(way, h, c).wait()


def reduce_scatter(n, dy, gate, up, w_gate, w_up, w_down):
    tokens, width = dy.shape
    units = gate.shape[1]
    rows, half = tokens // n, width // 2
    pieces = half // TILE
    block = (rows // 2, TILE)
    wide = jax.ShapeDtypeStruct((tokens, units), BF16)
    part = jax.ShapeDtypeStruct((rows, half), BF16)
    dma = pltpu.SemaphoreType.DMA
    return pl.pallas_call(
        functools.partial(reduce_kernel, n),
        out_shape=(wide, wide, wide, part, part, part, part, jax.ShapeDtypeStruct((units, width), BF16)),
        in_specs=[pl.BlockSpec(memory_space=pltpu.MemorySpace.HBM)] * 6,
        out_specs=[pl.BlockSpec(memory_space=pltpu.MemorySpace.HBM)] * 8,
        scratch_shapes=[
            pltpu.VMEM((units, width), BF16),
            pltpu.VMEM((width, 2 * units), BF16),
            pltpu.VMEM((n - 1, rows, 2 * units), BF16),
            pltpu.VMEM((2, rows, width), BF16),
            pltpu.VMEM((2, rows, units), BF16),
            pltpu.VMEM((2, rows, units), BF16),
            pltpu.VMEM(block, F32),
            pltpu.VMEM(block, F32),
            pltpu.VMEM((2, 2 * pieces, *block), BF16),
            pltpu.VMEM((2, n - 1, 2 * pieces, *block), BF16),
            pltpu.VMEM((2, pieces, *block), F32),
            pltpu.VMEM((2, 2 * pieces, *block), BF16),
            dma((units // TILE,)),
            dma((2, width // TILE)),
            dma((2, 2)),
            dma((2, 2, units // TILE)),
            dma((2, 2, units // TILE)),
            dma((2, 2)),
            dma((2, n - 1, 2)),
            dma((2, 2 * pieces)),
            dma((2, n - 1, 2 * pieces)),
            dma((2, n - 1, 2 * pieces)),
            dma((n + 2,)),
            dma((4,)),
            dma((2, 2 * pieces)),
            dma((2, 2 * pieces)),
            dma((2, 2 * pieces)),
        ],
        compiler_params=pltpu.CompilerParams(
            collective_id=0, has_side_effects=True, vmem_limit_bytes=VMEM_LIMIT
        ),
        cost_estimate=pl.CostEstimate(
            flops=8 * tokens * width * units, bytes_accessed=96 << 20, transcendentals=0
        ),
        name="reduce",
    )(dy, gate, up, w_gate, w_up, w_down)


def place_copies(n, hop, pieces, dx, bufs, in_sem, out_sem):
    me = lax.axis_index("tp")
    shards = (lax.rem(me + n - hop, n), lax.rem(me + 2 + hop, n))
    rows, half = pieces[0].shape
    ins, outs = [], []
    for way in range(2):
        at = (pl.ds(shards[way] * rows, rows), pl.ds(way * half, half))
        ins.append(pltpu.make_async_copy(pieces[way], bufs.at[way], in_sem.at[way]))
        outs.append(pltpu.make_async_copy(bufs.at[way], dx.at[at], out_sem.at[way]))
    return ins, outs


def weight_kernel(n, hops, a, b, down, *rest):
    pieces, rest = rest[: 2 * len(hops)], rest[-15:]
    out, dx, d_down, av, bv, ov, acc, bufs, dbuf, first_sem, b_sem, o_sem, in_sem, out_sem, d_sem = rest
    depth, height, cols = av.shape[0], av.shape[1] // 2, ov.shape[2]
    chunk = depth // FIRST
    blocks = bv.shape[1] // cols
    ins, outs = [], []
    for i, hop in enumerate(hops):
        two = place_copies(n, hop, pieces[2 * i : 2 * i + 2], dx, bufs.at[i], in_sem.at[i], out_sem.at[i])
        ins, outs = ins + two[0], outs + two[1]
    at = pl.ds((hops[0] // 2) * dbuf.shape[0], dbuf.shape[0])
    ins.append(pltpu.make_async_copy(down.at[at, :], dbuf, d_sem.at[0]))
    outs.append(pltpu.make_async_copy(dbuf, d_down.at[at, :], d_sem.at[1]))

    def first_copies(k):
        row = pl.ds(k * chunk, chunk)
        ha, hb = (row, pl.ds(0, height)), (row, pl.ds(0, cols))
        return (
            pltpu.make_async_copy(a.at[ha], av.at[ha], first_sem.at[0, k]),
            pltpu.make_async_copy(b.at[hb], bv.at[hb], first_sem.at[1, k]),
        )

    def b_copy(j):
        at = (slice(None), pl.ds(pl.multiple_of(j * cols, cols), cols))
        return pltpu.make_async_copy(b.at[at], bv.at[at], b_sem.at[j])

    def a_copy():
        at = (slice(None), pl.ds(height, height))
        return pltpu.make_async_copy(a.at[at], av.at[at], b_sem.at[0])

    def out_copy(block):
        i, j = block // blocks, lax.rem(block, blocks)
        at = (pl.ds(pl.multiple_of(i * height, height), height), pl.ds(pl.multiple_of(j * cols, cols), cols))
        slot = lax.rem(block, 2)
        return pltpu.make_async_copy(ov.at[slot], out.at[at], o_sem.at[slot])

    for k in range(2):
        for c in first_copies(k):
            c.start()
    for k in range(FIRST):
        for c in first_copies(k):
            c.wait()
        if k + 2 < FIRST:
            for c in first_copies(k + 2):
                c.start()
        elif k + 2 == FIRST:
            for j in range(1, blocks):
                b_copy(j).start()
        else:
            a_copy().start()
            for c in ins:
                c.start()
        row = pl.ds(k * chunk, chunk)
        part = dot(av[row, pl.ds(0, height)], bv[row, pl.ds(0, cols)], TN)
        if k == 0:
            acc[...] = part
        elif k + 1 < FIRST:
            acc[...] += part
        else:
            ov[0] = (acc[...] + part).astype(BF16)
    out_copy(0).start()

    def step(block, carry):
        i, j = block // blocks, lax.rem(block, blocks)

        @pl.when(block < blocks)
        def _():
            b_copy(j).wait()

        @pl.when(block == blocks)
        def _():
            a_copy().wait()
            for c in ins:
                c.wait()
            for c in outs:
                c.start()

        @pl.when(block >= 2)
        def _():
            out_copy(block - 2).wait()

        ha = pl.ds(pl.multiple_of(i * height, height), height)
        hb = pl.ds(pl.multiple_of(j * cols, cols), cols)
        ov[lax.rem(block, 2)] = dot(av[:, ha], bv[:, hb], TN).astype(BF16)
        out_copy(block).start()
        return carry

    lax.fori_loop(1, 2 * blocks, step, 0)
    for block in (2 * blocks - 2, 2 * blocks - 1):
        out_copy(block).wait()
    for c in outs:
        c.wait()


def weight_gradient(n, hops, a, b, down, pieces, old, limit, name):
    tokens, rows, cols = a.shape[0], a.shape[1], b.shape[1]
    anywhere = pl.BlockSpec(memory_space=pltpu.MemorySpace.HBM)
    shapes = ((rows, cols), (tokens, 2 * pieces[0].shape[1]), down.shape)
    args = (a, b, down, *pieces, *old)
    dma = pltpu.SemaphoreType.DMA
    return pl.pallas_call(
        functools.partial(weight_kernel, n, hops),
        out_shape=tuple(jax.ShapeDtypeStruct(shape, BF16) for shape in shapes),
        in_specs=[anywhere] * len(args),
        out_specs=[anywhere] * 3,
        scratch_shapes=[
            pltpu.VMEM((tokens, rows), BF16),
            pltpu.VMEM((tokens, cols), BF16),
            pltpu.VMEM((2, rows // 2, WIDE), BF16),
            pltpu.VMEM((rows // 2, WIDE), F32),
            pltpu.VMEM((len(hops), 2, *pieces[0].shape), BF16),
            pltpu.VMEM((down.shape[0] // 2, down.shape[1]), BF16),
            dma((2, FIRST)),
            dma((cols // WIDE,)),
            dma((2,)),
            dma((len(hops), 2)),
            dma((len(hops), 2)),
            dma((2,)),
        ],
        input_output_aliases={len(args) - 2 + i: 1 + i for i in range(len(old))},
        compiler_params=pltpu.CompilerParams(vmem_limit_bytes=limit),
        cost_estimate=pl.CostEstimate(
            flops=2 * tokens * rows * cols, bytes_accessed=48 << 20, transcendentals=0
        ),
        name=name,
    )(*args)


def finish_kernel(n, hop, a, b, _, dx, sem):
    me = lax.axis_index("tp")
    rows, half = a.shape
    copies = []
    for way, (piece, shard) in enumerate(((a, lax.rem(me + n - hop, n)), (b, lax.rem(me + 2 + hop, n)))):
        there = (pl.ds(shard * rows, rows), pl.ds(way * half, half))
        copies.append(pltpu.make_async_copy(piece, dx.at[there], sem.at[way]))
    for c in copies:
        c.start()
    for c in copies:
        c.wait()


def finish(n, hop, pieces, dx):
    anywhere = pl.BlockSpec(memory_space=pltpu.MemorySpace.HBM)
    near = pl.BlockSpec(memory_space=pltpu.MemorySpace.VMEM)
    return pl.pallas_call(
        functools.partial(finish_kernel, n, hop),
        out_shape=jax.ShapeDtypeStruct(dx.shape, BF16),
        in_specs=[near, near, anywhere],
        out_specs=anywhere,
        scratch_shapes=[pltpu.SemaphoreType.DMA((2,))],
        input_output_aliases={2: 0},
        compiler_params=pltpu.CompilerParams(vmem_limit_bytes=16 << 20),
        name="finish",
    )(*pieces, dx)


def solution(mesh):
    n = mesh.shape["tp"]
    to_right = [(i, (i + 1) % n) for i in range(n)]
    to_left = [(i, (i - 1) % n) for i in range(n)]

    def step(x, dy, gate, up, w_gate, w_up, w_down):
        d_gate, d_up, _, *parts, down = reduce_scatter(n, dy, gate, up, w_gate, w_up, w_down)
        own, pieces = parts[:2], parts[2:]

        def onward(pieces):
            return [lax.ppermute(p, "tp", ways) for p, ways in zip(pieces, (to_right, to_left))]

        later = onward(pieces)
        dw_gate, *old = weight_gradient(n, (0, 1), x, d_gate, down, (*own, *pieces), (), VMEM_LIMIT, "weight0")
        last = onward(later)
        dw_up, dx, dw_down = weight_gradient(n, (2,), x, d_up, down, later, old, 44 << 20, "weight1")
        return finish(n, n - 1, last, dx), dw_gate, dw_up, dw_down

    tokens, columns, rows = P("dp", None), P(None, "tp"), P("tp", None)
    return jax.shard_map(
        step,
        mesh=mesh,
        in_specs=(tokens, tokens, P("dp", "tp"), P("dp", "tp"), columns, columns, rows),
        out_specs=(tokens, P("dp", "tp"), P("dp", "tp"), P(("dp", "tp"), None)),
        check_vma=False,
    )
```
